32 devices in a mesh: rep: 1 (over z), dp: 4 (over y), sp: 8 (over x, core).
Axes of the slice: x: 4, y: 4, z: 1, core: 2. Of those that a mesh axis runs over, the one named last changes fastest.
The devices are a block of a 4x4x8 slice.
Arguments:
- hidden: bfloat16 [256, 4096], P(('rep', 'dp'))
- w_query: bfloat16 [4096, 4096], replicated
- w_key: bfloat16 [4096, 256], replicated
- w_value: bfloat16 [4096, 256], replicated
- w_out: bfloat16 [4096, 4096], P('sp')
- k_cache: bfloat16 [256, 2048, 1, 256], P(('rep', 'dp'), 'sp')
- v_cache: bfloat16 [256, 2048, 1, 256], P(('rep', 'dp'), 'sp')
- write_pos: int32 [256], P(('rep', 'dp'))
- valid_len: int32 [256], P(('rep', 'dp'))
Outputs:
- output 1: bfloat16 [256, 4096], P(('rep', 'dp'))
- output 2: bfloat16 [256, 2048, 1, 256], P(('rep', 'dp'), 'sp')
- output 3: bfloat16 [256, 2048, 1, 256], P(('rep', 'dp'), 'sp')
All inputs are finite; a program needn't handle non-finite values.
Results may differ from the reference program's by a relative error of at most 0.00650376.
Values are sent between devices in bfloat16 or wider.
A program may use at most 768 MiB of HBM per device.

```python
import jax
import jax.numpy as jnp
from jax import lax

MODEL_DIM = 4096
NUM_HEADS = 16
KV_HEADS = 1
HEAD_DIM = 256
BATCH_SIZE = 256
CACHE_LEN = 2048
SEGMENTS = 32


def draw_lengths(rng_key):
    keys = jax.random.split(rng_key, 3)
    shortest = CACHE_LEN // 4
    write_pos = jax.random.randint(keys[0], (BATCH_SIZE,), shortest - 1, CACHE_LEN, jnp.int32)
    long_row = jax.random.randint(keys[1], (), 0, BATCH_SIZE, jnp.int32)
    short_row = (long_row + 1 + jax.random.randint(keys[2], (), 0, BATCH_SIZE - 1, jnp.int32)) % BATCH_SIZE
    row_ids = jnp.arange(BATCH_SIZE, dtype=jnp.int32)
    write_pos = jnp.where(row_ids == long_row, CACHE_LEN - 1, write_pos)
    write_pos = jnp.where(row_ids == short_row, shortest - 1, write_pos)
    return write_pos, write_pos + 1


def setup_inputs(seed: int = 0, part: int = 0) -> dict:
    root = jax.random.key(seed)
    shared = jax.random.split(root, 4)
    own = jax.random.split(jax.random.fold_in(root, part), 8)
    seg_len = CACHE_LEN // SEGMENTS
    proj_width = NUM_HEADS * HEAD_DIM
    kv_width = KV_HEADS * HEAD_DIM
    w_query = (jax.random.normal(shared[0], (MODEL_DIM, proj_width), jnp.float32) * MODEL_DIM ** -0.5).astype(jnp.bfloat16)
    w_key = (jax.random.normal(shared[1], (MODEL_DIM, kv_width), jnp.float32) * MODEL_DIM ** -0.5).astype(jnp.bfloat16)
    w_value = (jax.random.normal(shared[2], (MODEL_DIM, kv_width), jnp.float32) * MODEL_DIM ** -0.5).astype(jnp.bfloat16)
    w_out = (jax.random.normal(shared[3], (proj_width, MODEL_DIM), jnp.float32) * proj_width ** -0.5).astype(jnp.bfloat16)
    hidden = jax.random.normal(own[0], (BATCH_SIZE, MODEL_DIM), jnp.float32).astype(jnp.bfloat16)
    cache_shape = (BATCH_SIZE, SEGMENTS, seg_len, KV_HEADS, HEAD_DIM)
    seg_shape = (BATCH_SIZE, SEGMENTS, 1, KV_HEADS, HEAD_DIM)
    flat_shape = (BATCH_SIZE, CACHE_LEN, KV_HEADS, HEAD_DIM)
    k_cache = (jax.random.normal(own[1], cache_shape, jnp.float32) + jax.random.normal(own[2], seg_shape, jnp.float32)).reshape(flat_shape).astype(jnp.bfloat16)
    v_cache = (jax.random.normal(own[3], cache_shape, jnp.float32) + jax.random.normal(own[4], seg_shape, jnp.float32)).reshape(flat_shape).astype(jnp.bfloat16)
    write_pos, valid_len = draw_lengths(own[5])
    return {'hidden': hidden, 'w_query': w_query, 'w_key': w_key, 'w_value': w_value, 'w_out': w_out, 'k_cache': k_cache, 'v_cache': v_cache, 'write_pos': write_pos, 'valid_len': valid_len}


def reference(hidden, w_query, w_key, w_value, w_out, k_cache, v_cache, write_pos, valid_len):
    group_size = NUM_HEADS // KV_HEADS
    query = jnp.dot(hidden, w_query, preferred_element_type=jnp.float32).astype(jnp.bfloat16)
    query = query.reshape(BATCH_SIZE, KV_HEADS, group_size, HEAD_DIM)
    key_new = jnp.dot(hidden, w_key, preferred_element_type=jnp.float32).astype(jnp.bfloat16)
    value_new = jnp.dot(hidden, w_value, preferred_element_type=jnp.float32).astype(jnp.bfloat16)
    positions = jnp.arange(CACHE_LEN, dtype=jnp.int32)
    at_pos = (positions[None, :] == write_pos[:, None])[:, :, None, None]
    k_next = jnp.where(at_pos, key_new.reshape(BATCH_SIZE, 1, KV_HEADS, HEAD_DIM), k_cache)
    v_next = jnp.where(at_pos, value_new.reshape(BATCH_SIZE, 1, KV_HEADS, HEAD_DIM), v_cache)

    def one_row(row_args):
        q_row, k_row, v_row, length = row_args
        scores = jnp.einsum('kgd,skd->kgs', q_row.astype(jnp.float32), k_row.astype(jnp.float32)) * HEAD_DIM ** -0.5
        scores = jnp.where(positions < length, scores, -jnp.inf)
        row_max = jnp.max(scores, axis=-1, keepdims=True)
        weights = jnp.exp(scores - row_max)
        total = jnp.sum(weights, axis=-1, keepdims=True)
        return jnp.einsum('kgs,skd->kgd', weights, v_row.astype(jnp.float32)) / total

    attention = lax.map(one_row, (query, k_next, v_next, valid_len))
    attention = attention.reshape(BATCH_SIZE, NUM_HEADS * HEAD_DIM).astype(jnp.bfloat16)
    attn_out = jnp.dot(attention, w_out, preferred_element_type=jnp.float32).astype(jnp.bfloat16)
    return (attn_out, k_next, v_next)
```

```python
import functools

import jax
import jax.numpy as jnp
from jax import lax
from jax.experimental import pallas as pl
from jax.experimental.pallas import tpu as pltpu
from jax.sharding import PartitionSpec as P

MESH = pl.DeviceIdType.MESH
NEG = -3.4e38
LANES = 128
F32 = jnp.float32
BF16 = jnp.bfloat16


def sp_dev(i):
    return {'sp': i}


def enter(n):
    me = lax.axis_index('sp')
    bar = pltpu.get_barrier_semaphore()
    for d in range(1, n):
        pl.semaphore_signal(bar, inc=1, device_id=sp_dev(lax.rem(me + d, n)), device_id_type=MESH)
    pl.semaphore_wait(bar, n - 1)


def rcopy(src, dst, ss, rs, dev):
    return pltpu.make_async_remote_copy(src_ref=src, dst_ref=dst, send_sem=ss, recv_sem=rs,
                                        device_id=sp_dev(dev), device_id_type=MESH)


def qkv_kernel(n, hid_hbm, wq_hbm, wk_hbm, wv_hbm, q_ref, kn_ref, vn_ref,
               hid, wq, wkv, hsem, wsem, ssem, rsem, psend, precv):
    nx = n // 2
    me = lax.axis_index('sp')
    x, c = me // 2, lax.rem(me, 2)
    cols = wq.shape[2]
    own = me
    opp = 2 * lax.rem(x + nx // 2, nx) + c
    partner = 2 * x + 1 - c
    ch = pltpu.make_async_copy(hid_hbm, hid, hsem)
    ch.start()
    blocks = (own, opp)
    loads = []
    for i, blk in enumerate(blocks):
        cp = pltpu.make_async_copy(wq_hbm.at[:, pl.ds(pl.multiple_of(blk * cols, cols), cols)], wq.at[i], wsem.at[i])
        cp.start()
        loads.append(cp)
    for i, w in enumerate((wk_hbm, wv_hbm)):
        cp = pltpu.make_async_copy(w, wkv.at[i], wsem.at[2 + i])
        cp.start()
        loads.append(cp)
    enter(n)
    ch.wait()

    def project(w):
        return jnp.dot(hid[...], w, preferred_element_type=F32).astype(BF16)

    loads[0].wait()
    q_ref[own] = project(wq[0])
    sends = [rcopy(q_ref.at[own], q_ref.at[own], psend.at[0], precv.at[0], partner)]
    for d in range(2):
        nb = lax.rem(x + (1 if d == 0 else nx - 1), nx)
        for t in range(2):
            sends.append(rcopy(q_ref.at[own], q_ref.at[own], ssem.at[d, t], rsem.at[d, c], 2 * nb + t))
    for s in sends[1:]:
        s.start()
    sends[0].start()
    loads[1].wait()
    q_ref[opp] = project(wq[1])
    po = rcopy(q_ref.at[opp], q_ref.at[opp], psend.at[1], precv.at[1], partner)
    po.start()
    sends.append(po)
    loads[2].wait()
    kn_ref[...] = project(wkv[0]).astype(F32)
    loads[3].wait()
    vn_ref[...] = project(wkv[1]).astype(F32)
    for s in sends:
        s.wait_send()
    pown, popp = partner, 2 * lax.rem(x + nx // 2, nx) + 1 - c
    rcopy(q_ref.at[own], q_ref.at[pown], psend.at[0], precv.at[0], partner).wait_recv()
    rcopy(q_ref.at[own], q_ref.at[popp], psend.at[1], precv.at[1], partner).wait_recv()
    for d in range(2):
        src = lax.rem(x + (nx - 1 if d == 0 else 1), nx)
        for t in range(2):
            rcopy(q_ref.at[own], q_ref.at[2 * src + t], ssem.at[d, t], rsem.at[d, t], partner).wait_recv()


def attn_kernel(group, scale, wp, vl, q_ref, kn_ref, vn_ref, k_hbm, v_hbm, ko_hbm, vo_hbm, acc_ref, ml_ref,
                kb, vb, qs, lsem, osem):
    rows, seq, hd = kb.shape
    heads = acc_ref.shape[1] // rows
    halves = hd // LANES
    steps = rows // group
    base = lax.axis_index('sp') * seq

    def load(g, start=True):
        s = pl.ds(g * group, group)
        return (pltpu.make_async_copy(k_hbm.at[s], kb.at[s], lsem.at[0, g]),
                pltpu.make_async_copy(v_hbm.at[s], vb.at[s], lsem.at[1, g]))

    def store(g):
        s = pl.ds(g * group, group)
        return (pltpu.make_async_copy(kb.at[s], ko_hbm.at[s], osem.at[0, g]),
                pltpu.make_async_copy(vb.at[s], vo_hbm.at[s], osem.at[1, g]))

    for g in range(steps):
        for cp in load(g):
            cp.start()
    per = q_ref.shape[2] // hd
    for h in range(heads):
        for z in range(halves):
            lo = (h % per) * hd + z * LANES
            qs[z, h * rows:(h + 1) * rows, :] = q_ref[h // per, :, lo:lo + LANES].astype(F32)

    pos_iota = lax.broadcasted_iota(jnp.int32, (heads, seq), 1)
    row_iota = lax.broadcasted_iota(jnp.int32, (16, hd), 0)
    lane_iota = lax.broadcasted_iota(jnp.int32, (heads, 128), 1)

    def put(buf, new, b, pos):
        start = pl.multiple_of((jnp.clip(pos, 0, seq - 1) // 16) * 16, 16)
        slab = buf[b, pl.ds(start, 16), :].astype(F32)
        row = jnp.broadcast_to(new[pl.ds(b, 1), :], slab.shape)
        buf[b, pl.ds(start, 16), :] = jnp.where(row_iota == pos - start, row, slab).astype(BF16)

    def step(g, carry):
        m_all, l_all = carry
        for cp in load(g):
            cp.wait()
        b0 = g * group
        for r in range(group):
            pos = wp[b0 + r] - base
            put(kb, kn_ref, b0 + r, pos)
            put(vb, vn_ref, b0 + r, pos)
        for cp in store(g):
            cp.start()
        scores = []
        for r in range(group):
            qb = jnp.concatenate([qs[z, pl.ds(b0 + r, heads, stride=rows), :] for z in range(halves)], axis=1).astype(BF16)
            scores.append(lax.dot_general(qb, kb[b0 + r], (((1,), (1,)), ((), ())), preferred_element_type=F32))
        probs = []
        for r in range(group):
            valid = pos_iota < vl[b0 + r] - base
            s = jnp.where(valid, scores[r] * scale, NEG)
            m = jnp.max(s, axis=1, keepdims=True)
            p = jnp.where(valid, jnp.exp(s - m), 0.0)
            l = jnp.sum(p, axis=1, keepdims=True)
            here = lane_iota == b0 + r
            m_all = jnp.where(here, m, m_all)
            l_all = jnp.where(here, l, l_all)
            probs.append(p.astype(BF16))
        for r in range(group):
            o = jnp.dot(probs[r], vb[b0 + r], preferred_element_type=F32)
            for z in range(halves):
                acc_ref[z, pl.ds(b0 + r, heads, stride=rows), :] = o[:, z * LANES:(z + 1) * LANES]
        return m_all, l_all

    m_all, l_all = lax.fori_loop(0, steps, step, (jnp.full((heads, 128), NEG, F32), jnp.zeros((heads, 128), F32)))
    for i in range(ml_ref.shape[0]):
        ml_ref[i, 0:per, :] = m_all[i * per:(i + 1) * per]
        ml_ref[i, per:2 * per, :] = l_all[i * per:(i + 1) * per]
    for g in range(steps):
        for cp in store(g):
            cp.wait()


def out_kernel(n, acc_ref, ml_ref, w_hbm, out_ref, wv, ra, rml, sb, sml, rb, rbml, sd, rd, se, re,
               wsem, asend, arecv, amsend, amrecv, bsend, brecv, bmsend, bmrecv, dsend, drecv, esend, erecv,
               fsend, frecv, gsend, grecv):
    nx = n // 2
    me = lax.axis_index('sp')
    x, c = me // 2, lax.rem(me, 2)
    partner = 2 * x + 1 - c
    wide = wv.shape[2]
    blk_rows = ra.shape[2]
    halves = acc_ref.shape[0]
    rows = out_ref.shape[0]
    per = blk_rows // rows
    order = [2, 1, 3, 0] if nx == 4 else list(range(1, nx)) + [0]

    wloads = []
    for j in range(n):
        cp = pltpu.make_async_copy(w_hbm.at[:, j * wide:(j + 1) * wide], wv.at[j], wsem.at[j])
        cp.start()
        wloads.append(cp)
    enter(n)

    def chip(d):
        return lax.rem(x + d, nx)

    def acc_at(j):
        return acc_ref.at[:, pl.ds(pl.multiple_of(j * blk_rows, blk_rows), blk_rows)]

    pending = []
    for d in order:
        j = 2 * chip(d) + 1 - c
        a = rcopy(acc_at(j), ra.at[d], asend.at[d], arecv.at[d], partner)
        b = rcopy(ml_ref.at[j], rml.at[d], amsend.at[d], amrecv.at[d], partner)
        b.start()
        a.start()
        pending += [a, b]
    for d in order:
        j = 2 * chip(d) + c
        rcopy(acc_at(j), ra.at[d], asend.at[d], arecv.at[d], partner).wait_recv()
        rcopy(ml_ref.at[j], rml.at[d], amsend.at[d], amrecv.at[d], partner).wait_recv()
        mine, theirs = ml_ref[j], rml[d]
        m = jnp.maximum(mine[0:per], theirs[0:per])
        ca, cb = jnp.exp(mine[0:per] - m), jnp.exp(theirs[0:per] - m)
        l = ca * mine[per:2 * per] + cb * theirs[per:2 * per]
        cols = jnp.transpose(jnp.concatenate([ca, cb, m, l], axis=0))
        sml[d, 0:per, :] = m
        sml[d, per:2 * per, :] = l
        for h in range(per):
            r = slice(h * rows, (h + 1) * rows)
            for z in range(halves):
                own = acc_ref[z, pl.ds(pl.multiple_of(j * blk_rows + h * rows, rows), rows), :]
                sb[d, z, r, :] = own * cols[0:rows, h:h + 1] + ra[d, z, r, :] * cols[0:rows, per + h:per + h + 1]
        if d:
            a = rcopy(sb.at[d], rb.at[d], bsend.at[d], brecv.at[d], j)
            b = rcopy(sml.at[d], rbml.at[d], bmsend.at[d], bmrecv.at[d], j)
            b.start()
            a.start()
            pending += [a, b]
    for d in range(1, nx):
        rcopy(sb.at[d], rb.at[d], bsend.at[d], brecv.at[d], me ^ 1).wait_recv()
        rcopy(sml.at[d], rbml.at[d], bmsend.at[d], bmrecv.at[d], me ^ 1).wait_recv()
    mls = [sml[0]] + [rbml[d] for d in range(1, nx)]
    m = functools.reduce(jnp.maximum, [t[0:per] for t in mls])
    cs = [jnp.exp(t[0:per] - m) for t in mls]
    l = sum(cf * t[per:2 * per] for cf, t in zip(cs, mls))
    cols = jnp.transpose(jnp.concatenate([cf / l for cf in cs], axis=0))
    heads = []
    for h in range(per):
        r = slice(h * rows, (h + 1) * rows)
        for z in range(halves):
            parts = [sb[0, z, r, :]] + [rb[d, z, r, :] for d in range(1, nx)]
            heads.append(sum(part * cols[0:rows, d * per + h:d * per + h + 1] for d, part in enumerate(parts)))
    attn = jnp.concatenate(heads, axis=1).astype(BF16)

    for cp in wloads:
        cp.wait()
    for d in order:
        sd[d] = jnp.dot(attn, wv[2 * chip(d) + 1 - c], preferred_element_type=F32)
        a = rcopy(sd.at[d], rd.at[d], dsend.at[d], drecv.at[d], partner)
        a.start()
        pending.append(a)
    for d in order:
        j = 2 * chip(d) + c
        part = jnp.dot(attn, wv[j], preferred_element_type=F32)
        rcopy(sd.at[d], rd.at[d], dsend.at[d], drecv.at[d], partner).wait_recv()
        se[d] = part + rd[d]
        if d:
            a = rcopy(se.at[d], re.at[d], esend.at[d], erecv.at[d], j)
            a.start()
            pending.append(a)
    for d in range(1, nx):
        rcopy(se.at[d], re.at[d], esend.at[d], erecv.at[d], partner).wait_recv()

    def out_at(j):
        return out_ref.at[:, pl.ds(pl.multiple_of(j * wide, wide), wide)]

    out_ref[:, pl.ds(pl.multiple_of(me * wide, wide), wide)] = (
        se[0] + sum(re[d] for d in range(1, nx))).astype(BF16)
    for d in order[:-1]:
        a = rcopy(out_at(me), out_at(me), fsend.at[d], frecv.at[d], 2 * chip(d) + c)
        a.start()
        pending.append(a)
    a = rcopy(out_at(me), out_at(me), gsend.at[0], grecv.at[0], partner)
    a.start()
    pending.append(a)
    near = order[1:-1] + order[:1]
    for d in near:
        src = 2 * chip(nx - d) + c
        rcopy(out_at(me), out_at(src), fsend.at[d], frecv.at[d], partner).wait_recv()
        a = rcopy(out_at(src), out_at(src), gsend.at[d], grecv.at[d], partner)
        a.start()
        pending.append(a)
    for d in [0] + near:
        src = 2 * chip(nx - d if d else 0) + 1 - c
        rcopy(out_at(me), out_at(src), gsend.at[d], grecv.at[d], partner).wait_recv()
    for a in pending:
        a.wait_send()


def solution(mesh):
    n = mesh.shape['sp']
    nx = n // 2
    row_spec = P(('rep', 'dp'), None)
    cache_spec = P(('rep', 'dp'), 'sp', None, None)
    len_spec = P(('rep', 'dp'))
    VM = pl.BlockSpec(memory_space=pltpu.VMEM)
    HB = pl.BlockSpec(memory_space=pltpu.HBM)
    SM = pl.BlockSpec(memory_space=pltpu.SMEM)
    DMA = pltpu.SemaphoreType.DMA

    def local_step(hidden, w_query, w_key, w_value, w_out, k_cache, v_cache, write_pos, valid_len):
        rows, seq, kv_heads, hd = k_cache.shape
        width = hidden.shape[1]
        proj = w_query.shape[1]
        heads = proj // hd
        cols = proj // n
        per = heads // n
        k3, v3 = k_cache.reshape(rows, seq, hd), v_cache.reshape(rows, seq, hd)
        sds = jax.ShapeDtypeStruct

        q, kn, vn = pl.pallas_call(
            functools.partial(qkv_kernel, n),
            out_shape=(sds((n, rows, cols), BF16), sds((rows, hd), F32), sds((rows, hd), F32)),
            in_specs=[HB] * 4, out_specs=(VM, VM, VM),
            scratch_shapes=[pltpu.VMEM((rows, width), BF16), pltpu.VMEM((2, width, cols), BF16),
                            pltpu.VMEM((2, width, hd), BF16), DMA, DMA((4,)), DMA((2, 2)), DMA((2, 2)),
                            DMA((2,)), DMA((2,))],
            compiler_params=pltpu.CompilerParams(collective_id=0, has_side_effects=True,
                                                 vmem_limit_bytes=32 * 2 ** 20),
            name='qkv',
        )(hidden, w_query, w_key, w_value)

        group = 8
        k_new, v_new, acc, ml = pl.pallas_call(
            functools.partial(attn_kernel, group, hd ** -0.5),
            out_shape=(sds((rows, seq, hd), BF16), sds((rows, seq, hd), BF16), sds((hd // LANES, heads * rows, LANES), F32),
                       sds((n, 8, 128), F32)),
            in_specs=[SM, SM, VM, VM, VM, HB, HB], out_specs=(HB, HB, VM, VM),
            scratch_shapes=[pltpu.VMEM((rows, seq, hd), BF16), pltpu.VMEM((rows, seq, hd), BF16),
                            pltpu.VMEM((hd // LANES, heads * rows, LANES), F32), DMA((2, rows // group)), DMA((2, rows // group))],
            compiler_params=pltpu.CompilerParams(vmem_limit_bytes=40 * 2 ** 20),
            name='attn',
        )(write_pos, valid_len, q, kn, vn, k3, v3)

        blk = per * rows
        wide = width // n
        f = pltpu.VMEM
        out = pl.pallas_call(
            functools.partial(out_kernel, n),
            out_shape=sds((rows, width), BF16),
            in_specs=[VM, VM, HB], out_specs=VM,
            scratch_shapes=[f((n, w_out.shape[0], wide), BF16),
                            f((nx, hd // LANES, blk, LANES), F32), f((nx, 8, 128), F32), f((nx, hd // LANES, blk, LANES), F32), f((nx, 8, 128), F32),
                            f((nx, hd // LANES, blk, LANES), F32), f((nx, 8, 128), F32),
                            f((nx, rows, wide), F32), f((nx, rows, wide), F32),
                            f((nx, rows, wide), F32), f((nx, rows, wide), F32),
                            DMA((n,))] + [DMA((nx,))] * 16,
            compiler_params=pltpu.CompilerParams(collective_id=1, has_side_effects=True,
                                                 vmem_limit_bytes=32 * 2 ** 20),
            name='outp',
        )(acc, ml, w_out)
        return out, k_new.reshape(k_cache.shape), v_new.reshape(v_cache.shape)

    return jax.shard_map(local_step, mesh=mesh,
                         in_specs=(row_spec, P(), P(), P(), P('sp', None), cache_spec, cache_spec, len_spec, len_spec),
                         out_specs=(row_spec, cache_spec, cache_spec), check_vma=False)
```

```python
import functools

import jax
import jax.numpy as jnp
from jax import lax
from jax.experimental import pallas as pl
from jax.experimental.pallas import tpu as pltpu
from jax.sharding import PartitionSpec as P

MESH = pl.DeviceIdType.MESH
NEG = -3.4e38
LANES = 128
F32 = jnp.float32
BF16 = jnp.bfloat16


def sp_dev(i):
    return {'sp': i}


def rcopy(src, dst, ss, rs, dev):
    return pltpu.make_async_remote_copy(src_ref=src, dst_ref=dst, send_sem=ss, recv_sem=rs,
                                        device_id=sp_dev(dev), device_id_type=MESH)


def qkv_kernel(n, hid_hbm, wq_hbm, wk_hbm, wv_hbm, k_hbm, v_hbm, q_ref, kv_ref, kb, vb,
               hid, wq, wkv, hsem, wsem, csem, ssem, rsem, psend, precv):
    nx = n // 2
    me = lax.axis_index('sp')
    x, c = me // 2, lax.rem(me, 2)
    cols = wq.shape[2]
    own = me
    opp = 2 * lax.rem(x + nx // 2, nx) + c
    partner = 2 * x + 1 - c
    ch = pltpu.make_async_copy(hid_hbm, hid, hsem)
    ch.start()
    loads = []
    for i, blk in enumerate((own, opp)):
        cp = pltpu.make_async_copy(wq_hbm.at[:, pl.ds(pl.multiple_of(blk * cols, cols), cols)], wq.at[i], wsem.at[i])
        cp.start()
        loads.append(cp)
    near = [lax.rem(x + d, nx) for d in (1, nx - 1)]
    bar = pltpu.get_barrier_semaphore()
    peers = [2 * t + u for t in near for u in range(2)] + [partner]
    for peer in peers:
        pl.semaphore_signal(bar, inc=1, device_id=sp_dev(peer), device_id_type=MESH)
    pick = [pltpu.make_async_copy(w, wkv, wsem.at[2]) for w in (wk_hbm, wv_hbm)]
    for i in range(2):
        @pl.when(c == i)
        def _():
            pick[i].start()
    ch.wait()
    loads[0].wait()
    parts = csem.shape[1]
    step = kb.shape[0] // parts
    caches = []
    for g in range(parts):
        for i, (src, dst) in enumerate(((k_hbm, kb), (v_hbm, vb))):
            cp = pltpu.make_async_copy(src.at[pl.ds(g * step, step)], dst.at[pl.ds(g * step, step)], csem.at[i, g])
            cp.start()
            caches.append(cp)

    def project(w):
        return jnp.dot(hid[...], w, preferred_element_type=F32).astype(BF16)

    q_ref[own] = project(wq[0])
    pl.semaphore_wait(bar, len(peers))
    sends = []
    for d in range(2):
        for t in range(2):
            sends.append(rcopy(q_ref.at[own], q_ref.at[own], ssem.at[d, t], rsem.at[d, c], 2 * near[d] + t))
    sends.append(rcopy(q_ref.at[own], q_ref.at[own], psend.at[0], precv.at[0], partner))
    for s in sends:
        s.start()
    loads[1].wait()
    q_ref[opp] = project(wq[1])
    sends.append(rcopy(q_ref.at[opp], q_ref.at[opp], psend.at[1], precv.at[1], partner))
    sends[-1].start()
    pick[0].wait()
    kv_ref[c] = project(wkv[...]).astype(F32)
    sends.append(rcopy(kv_ref.at[c], kv_ref.at[c], psend.at[2], precv.at[2], partner))
    sends[-1].start()
    for s in sends:
        s.wait_send()
    popp = 2 * lax.rem(x + nx // 2, nx) + 1 - c
    rcopy(q_ref.at[own], q_ref.at[partner], psend.at[0], precv.at[0], partner).wait_recv()
    rcopy(q_ref.at[own], q_ref.at[popp], psend.at[1], precv.at[1], partner).wait_recv()
    rcopy(kv_ref.at[c], kv_ref.at[1 - c], psend.at[2], precv.at[2], partner).wait_recv()
    for d in range(2):
        for t in range(2):
            rcopy(q_ref.at[own], q_ref.at[2 * near[1 - d] + t], ssem.at[d, t], rsem.at[d, t], partner).wait_recv()
    for cp in caches:
        cp.wait()


def attn_kernel(group, chunk, scale, wp, vl, q_ref, kv_ref, k_in, v_in, ko_hbm, vo_hbm, kb, vb, acc_ref, ml_ref,
                qs, osem):
    del k_in, v_in
    rows, seq, hd = kb.shape
    heads = acc_ref.shape[1] // rows
    halves = hd // LANES
    steps = rows // group
    base = lax.axis_index('sp') * seq

    def store(g):
        s = pl.ds(g * group, group)
        return (pltpu.make_async_copy(kb.at[s], ko_hbm.at[s], osem.at[0, g]),
                pltpu.make_async_copy(vb.at[s], vo_hbm.at[s], osem.at[1, g]))

    per = q_ref.shape[2] // hd
    row_iota = lax.broadcasted_iota(jnp.int32, (16, hd), 0)

    def put(buf, i, b, pos):
        start = pl.multiple_of((jnp.clip(pos, 0, seq - 1) // 16) * 16, 16)
        slab = buf[b, pl.ds(start, 16), :].astype(F32)
        row = jnp.broadcast_to(kv_ref[i, pl.ds(b, 1), :], slab.shape)
        buf[b, pl.ds(start, 16), :] = jnp.where(row_iota == pos - start, row, slab).astype(BF16)

    def update(g, carry):
        for r in range(group):
            pos = wp[g * group + r] - base
            put(kb, 0, g * group + r, pos)
            put(vb, 1, g * group + r, pos)
        for cp in store(g):
            cp.start()
        return carry

    lax.fori_loop(0, steps, update, 0)
    for h in range(heads):
        for z in range(halves):
            lo = (h % per) * hd + z * LANES
            for t in range(rows // chunk):
                to = (t * heads + h) * chunk
                qs[z, to:to + chunk, :] = q_ref[h // per, t * chunk:(t + 1) * chunk, lo:lo + LANES].astype(F32)

    pos_iota = lax.broadcasted_iota(jnp.int32, (heads, seq), 1)
    lane_iota = lax.broadcasted_iota(jnp.int32, (heads, LANES), 1)

    def step(g, carry):
        m_all, l_all = carry
        b0 = g * group
        at0 = (b0 // chunk) * (heads * chunk) + lax.rem(b0, chunk)
        scores = []
        for r in range(group):
            qb = jnp.concatenate([qs[z, pl.ds(at0 + r, heads, stride=chunk), :] for z in range(halves)], axis=1)
            scores.append(lax.dot_general(qb.astype(BF16), kb[b0 + r], (((1,), (1,)), ((), ())),
                                          preferred_element_type=F32))
        probs = []
        for r in range(group):
            valid = pos_iota < vl[b0 + r] - base
            s = jnp.where(valid, scores[r] * scale, NEG)
            m = jnp.max(s, axis=1, keepdims=True)
            p = jnp.where(valid, jnp.exp(s - m), 0.0)
            l = jnp.sum(p, axis=1, keepdims=True)
            here = lane_iota == b0 + r
            m_all = jnp.where(here, m, m_all)
            l_all = jnp.where(here, l, l_all)
            probs.append(p.astype(BF16))
        for r in range(group):
            o = jnp.dot(probs[r], vb[b0 + r], preferred_element_type=F32)
            for z in range(halves):
                acc_ref[z, pl.ds(at0 + r, heads, stride=chunk), :] = o[:, z * LANES:(z + 1) * LANES]
        return m_all, l_all

    m_all, l_all = lax.fori_loop(0, steps, step, (jnp.full((heads, LANES), NEG, F32), jnp.zeros((heads, LANES), F32)))
    for i in range(ml_ref.shape[0]):
        ml_ref[i, 0:per, :] = m_all[i * per:(i + 1) * per]
        ml_ref[i, per:2 * per, :] = l_all[i * per:(i + 1) * per]
    for g in range(steps):
        for cp in store(g):
            cp.wait()


def out_kernel(n, acc_ref, ml_ref, w_ref, out_ref, ra, rml, ca, sb, sml, rb, rbml, cb, sd, rd, se, re,
               amsend, amrecv, bmsend, bmrecv, asend, arecv, bsend, brecv, dsend, drecv, esend, erecv,
               fsend, frecv, gsend, grecv):
    nx = n // 2
    me = lax.axis_index('sp')
    x, c = me // 2, lax.rem(me, 2)
    partner = 2 * x + 1 - c
    wide = out_ref.shape[1] // n
    halves = acc_ref.shape[0]
    chunks, blk = ra.shape[0], ra.shape[3]
    chunk = out_ref.shape[0] // chunks
    per = blk // chunk
    far = [2, 1, 3] if nx == 4 else list(range(1, nx))
    near = [1, 3, 2] if nx == 4 else list(range(1, nx))
    order = far + [0]

    def chip(d):
        return lax.rem(x + d, nx)

    bar = pltpu.get_barrier_semaphore()
    peers = [2 * chip(d) + c for d in range(1, nx)] + [partner]
    for peer in peers:
        pl.semaphore_signal(bar, inc=1, device_id=sp_dev(peer), device_id_type=MESH)
    pl.semaphore_wait(bar, len(peers))

    def acc_at(t, j):
        return pl.ds(pl.multiple_of((t * n + j) * blk, blk), blk)

    pending = []

    def go(*args):
        cp = rcopy(*args)
        cp.start()
        pending.append(cp)

    def landed(*args):
        rcopy(*args, partner).wait_recv()

    for d in order:
        go(ml_ref.at[2 * chip(d) + 1 - c], rml.at[d], amsend.at[d], amrecv.at[d], partner)
    for t in range(chunks):
        for d in order:
            go(acc_ref.at[:, acc_at(t, 2 * chip(d) + 1 - c)], ra.at[t, d], asend.at[t, d], arecv.at[t, d], partner)
    for d in order:
        j = 2 * chip(d) + c
        landed(ml_ref.at[j], rml.at[d], amsend.at[d], amrecv.at[d])
        mine, theirs = ml_ref[j], rml[d]
        m = jnp.maximum(mine[0:per], theirs[0:per])
        fa, fb = jnp.exp(mine[0:per] - m), jnp.exp(theirs[0:per] - m)
        l = fa * mine[per:2 * per] + fb * theirs[per:2 * per]
        ca[d] = jnp.transpose(jnp.concatenate([fa, fb, m, l], axis=0))
        sml[d, 0:per, :] = m
        sml[d, per:2 * per, :] = l
        if d:
            go(sml.at[d], rbml.at[d], bmsend.at[d], bmrecv.at[d], j)
    for t in range(chunks):
        for d in order:
            j = 2 * chip(d) + c
            landed(ra.at[t, d], ra.at[t, d], asend.at[t, d], arecv.at[t, d])
            for h in range(per):
                r = slice(h * chunk, (h + 1) * chunk)
                f = ca[d, t * chunk:(t + 1) * chunk, :]
                for z in range(halves):
                    own = acc_ref[z, pl.ds(pl.multiple_of((t * n + j) * blk + h * chunk, chunk), chunk), :]
                    sb[t, d, z, r, :] = own * f[:, h:h + 1] + ra[t, d, z, r, :] * f[:, per + h:per + h + 1]
            if d:
                go(sb.at[t, d], rb.at[t, d], bsend.at[t, d], brecv.at[t, d], j)
    for d in range(1, nx):
        landed(sml.at[d], rbml.at[d], bmsend.at[d], bmrecv.at[d])
    mls = [sml[0]] + [rbml[d] for d in range(1, nx)]
    m = functools.reduce(jnp.maximum, [u[0:per] for u in mls])
    fs = [jnp.exp(u[0:per] - m) for u in mls]
    l = sum(f * u[per:2 * per] for f, u in zip(fs, mls))
    cb[...] = jnp.transpose(jnp.concatenate([f / l for f in fs], axis=0))

    def w_at(j):
        return w_ref[:, pl.ds(pl.multiple_of(j * wide, wide), wide)]

    def out_at(t, j):
        return out_ref.at[pl.ds(t * chunk, chunk), pl.ds(pl.multiple_of(j * wide, wide), wide)]

    def project(t):
        for d in range(1, nx):
            landed(sb.at[t, d], rb.at[t, d], bsend.at[t, d], brecv.at[t, d])
        f = cb[t * chunk:(t + 1) * chunk, :]
        heads = []
        for h in range(per):
            r = slice(h * chunk, (h + 1) * chunk)
            for z in range(halves):
                terms = [sb[t, 0, z, r, :]] + [rb[t, d, z, r, :] for d in range(1, nx)]
                heads.append(sum(u * f[:, d * per + h:d * per + h + 1] for d, u in enumerate(terms)))
        attn = jnp.concatenate(heads, axis=1).astype(BF16)
        for d in order:
            sd[t, d] = jnp.dot(attn, w_at(2 * chip(d) + 1 - c), preferred_element_type=F32)
            go(sd.at[t, d], rd.at[t, d], dsend.at[t, d], drecv.at[t, d], partner)
        for d in order:
            se[t, d] = jnp.dot(attn, w_at(2 * chip(d) + c), preferred_element_type=F32)
        for d in order:
            landed(sd.at[t, d], rd.at[t, d], dsend.at[t, d], drecv.at[t, d])
            se[t, d] = se[t, d] + rd[t, d]
            if d:
                go(se.at[t, d], re.at[t, d], esend.at[t, d], erecv.at[t, d], 2 * chip(d) + c)

    def finish(t):
        for d in range(1, nx):
            landed(se.at[t, d], re.at[t, d], esend.at[t, d], erecv.at[t, d])
        out_ref[t * chunk:(t + 1) * chunk, pl.ds(pl.multiple_of(me * wide, wide), wide)] = (
            se[t, 0] + sum(re[t, d] for d in range(1, nx))).astype(BF16)
        for d in far:
            go(out_at(t, me), out_at(t, me), fsend.at[t, d], frecv.at[t, d], 2 * chip(d) + c)
        go(out_at(t, me), out_at(t, me), gsend.at[t, 0], grecv.at[t, 0], partner)

    def forward(t):
        for d in near:
            src = 2 * chip(nx - d) + c
            landed(out_at(t, me), out_at(t, src), fsend.at[t, d], frecv.at[t, d])
            go(out_at(t, src), out_at(t, src), gsend.at[t, d], grecv.at[t, d], partner)

    for t in range(chunks):
        project(t)
        if t >= 2:
            finish(t - 2)
    finish(chunks - 2)
    for t in range(chunks - 2):
        forward(t)
    finish(chunks - 1)
    forward(chunks - 2)
    forward(chunks - 1)
    for t in range(chunks):
        for d in [0] + near:
            src = 2 * chip(nx - d if d else 0) + 1 - c
            landed(out_at(t, me), out_at(t, src), gsend.at[t, d], grecv.at[t, d])
    for cp in pending:
        cp.wait_send()


def solution(mesh):
    n = mesh.shape['sp']
    nx = n // 2
    row_spec = P(('rep', 'dp'), None)
    cache_spec = P(('rep', 'dp'), 'sp', None, None)
    len_spec = P(('rep', 'dp'))
    VM = pl.BlockSpec(memory_space=pltpu.VMEM)
    HB = pl.BlockSpec(memory_space=pltpu.HBM)
    SM = pl.BlockSpec(memory_space=pltpu.SMEM)
    DMA = pltpu.SemaphoreType.DMA

    def local_step(hidden, w_query, w_key, w_value, w_out, k_cache, v_cache, write_pos, valid_len):
        rows, seq, kv_heads, hd = k_cache.shape
        width = hidden.shape[1]
        proj = w_query.shape[1]
        heads = proj // hd
        cols = proj // n
        per = heads // n
        k3, v3 = k_cache.reshape(rows, seq, hd), v_cache.reshape(rows, seq, hd)
        sds = jax.ShapeDtypeStruct

        group, chunk = 8, rows // 4
        chunks = rows // chunk
        f = pltpu.VMEM
        q, kv, kb, vb = pl.pallas_call(
            functools.partial(qkv_kernel, n),
            out_shape=(f((n, rows, cols), BF16), f((2, rows, hd), F32),
                       f((rows, seq, hd), BF16), f((rows, seq, hd), BF16)),
            in_specs=[HB] * 6, out_specs=(VM,) * 4,
            scratch_shapes=[f((rows, width), BF16), f((2, width, cols), BF16), f((width, hd), BF16),
                            DMA, DMA((3,)), DMA((2, 4)), DMA((2, 2)), DMA((2, 2)), DMA((3,)), DMA((3,))],
            compiler_params=pltpu.CompilerParams(collective_id=0, has_side_effects=True,
                                                 vmem_limit_bytes=46 * 2 ** 20),
            name='qkv',
        )(hidden, w_query, w_key, w_value, k3, v3)

        accs = f((hd // LANES, heads * rows, LANES), F32)
        k_new, v_new, _, _, acc, ml = pl.pallas_call(
            functools.partial(attn_kernel, group, chunk, hd ** -0.5),
            out_shape=(sds((rows, seq, hd), BF16), sds((rows, seq, hd), BF16), f((rows, seq, hd), BF16),
                       f((rows, seq, hd), BF16), accs, f((n, 8, LANES), F32)),
            in_specs=[SM, SM, VM, VM, VM, VM], out_specs=(HB, HB, VM, VM, VM, VM),
            scratch_shapes=[f(accs.shape, F32), DMA((2, rows // group))],
            input_output_aliases={4: 2, 5: 3},
            compiler_params=pltpu.CompilerParams(vmem_limit_bytes=16 * 2 ** 20),
            name='attn',
        )(write_pos, valid_len, q, kv, kb, vb)

        wide = width // n
        pair = (chunks, nx, hd // LANES, per * chunk, LANES)
        sums = (chunks, nx, chunk, wide)
        mls = (nx, 8, LANES)
        out = pl.pallas_call(
            functools.partial(out_kernel, n),
            out_shape=sds((rows, width), BF16),
            in_specs=[VM, VM, VM], out_specs=VM,
            scratch_shapes=[f(pair, F32), f(mls, F32), f((nx, LANES, 8), F32), f(pair, F32), f(mls, F32),
                            f(pair, F32), f(mls, F32), f((LANES, 8), F32),
                            f(sums, F32), f(sums, F32), f(sums, F32), f(sums, F32),
                            ] + [DMA((nx,))] * 4 + [DMA((chunks, nx))] * 12,
            compiler_params=pltpu.CompilerParams(collective_id=1, has_side_effects=True,
                                                 vmem_limit_bytes=20 * 2 ** 20),
            name='outp',
        )(acc, ml, w_out)
        return out, k_new.reshape(k_cache.shape), v_new.reshape(v_cache.shape)

    return jax.shard_map(local_step, mesh=mesh,
                         in_specs=(row_spec, P(), P(), P(), P('sp', None), cache_spec, cache_spec, len_spec, len_spec),
                         out_specs=(row_spec, cache_spec, cache_spec), check_vma=False)
```

```python
import functools

import jax
import jax.numpy as jnp
from jax import lax
from jax.experimental import pallas as pl
from jax.experimental.pallas import tpu as pltpu
from jax.sharding import PartitionSpec as P

MESH = pl.DeviceIdType.MESH
NEG = -3.4e38
LANES = 128
F32 = jnp.float32
BF16 = jnp.bfloat16


def sp_dev(i):
    return {'sp': i}


def rcopy(src, dst, ss, rs, dev):
    return pltpu.make_async_remote_copy(src_ref=src, dst_ref=dst, send_sem=ss, recv_sem=rs,
                                        device_id=sp_dev(dev), device_id_type=MESH)


def qkv_kernel(n, hid_hbm, wq_hbm, wk_hbm, wv_hbm, k_hbm, v_hbm, q_ref, kv_ref, kb, vb,
               hid, wq, wkv, hsem, wsem, csem, ssem, rsem, psend, precv):
    nx = n // 2
    me = lax.axis_index('sp')
    x, c = me // 2, lax.rem(me, 2)
    cols = wq.shape[2]
    own = me
    opp = 2 * lax.rem(x + nx // 2, nx) + c
    partner = 2 * x + 1 - c
    ch = pltpu.make_async_copy(hid_hbm, hid, hsem)
    ch.start()
    loads = []
    for i, blk in enumerate((own, opp)):
        cp = pltpu.make_async_copy(wq_hbm.at[:, pl.ds(pl.multiple_of(blk * cols, cols), cols)], wq.at[i], wsem.at[i])
        cp.start()
        loads.append(cp)
    near = [lax.rem(x + d, nx) for d in (1, nx - 1)]
    bar = pltpu.get_barrier_semaphore()
    peers = [2 * t + u for t in near for u in range(2)] + [partner]
    for peer in peers:
        pl.semaphore_signal(bar, inc=1, device_id=sp_dev(peer), device_id_type=MESH)
    pick = [pltpu.make_async_copy(w, wkv, wsem.at[2]) for w in (wk_hbm, wv_hbm)]
    for i in range(2):
        @pl.when(c == i)
        def _():
            pick[i].start()
    ch.wait()
    loads[0].wait()
    parts = csem.shape[1]
    step = kb.shape[0] // parts
    caches = []
    for g in range(parts):
        for i, (src, dst) in enumerate(((k_hbm, kb), (v_hbm, vb))):
            cp = pltpu.make_async_copy(src.at[pl.ds(g * step, step)], dst.at[pl.ds(g * step, step)], csem.at[i, g])
            cp.start()
            caches.append(cp)

    def project(w):
        return jnp.dot(hid[...], w, preferred_element_type=F32).astype(BF16)

    q_ref[own] = project(wq[0])
    pl.semaphore_wait(bar, len(peers))
    sends = []
    for d in range(2):
        for t in range(2):
            sends.append(rcopy(q_ref.at[own], q_ref.at[own], ssem.at[d, t], rsem.at[d, c], 2 * near[d] + t))
    sends.append(rcopy(q_ref.at[own], q_ref.at[own], psend.at[0], precv.at[0], partner))
    for s in sends:
        s.start()
    loads[1].wait()
    q_ref[opp] = project(wq[1])
    sends.append(rcopy(q_ref.at[opp], q_ref.at[opp], psend.at[1], precv.at[1], partner))
    sends[-1].start()
    pick[0].wait()
    kv_ref[c] = project(wkv[...]).astype(F32)
    sends.append(rcopy(kv_ref.at[c], kv_ref.at[c], psend.at[2], precv.at[2], partner))
    sends[-1].start()
    for s in sends:
        s.wait_send()
    popp = 2 * lax.rem(x + nx // 2, nx) + 1 - c
    rcopy(q_ref.at[own], q_ref.at[partner], psend.at[0], precv.at[0], partner).wait_recv()
    rcopy(q_ref.at[own], q_ref.at[popp], psend.at[1], precv.at[1], partner).wait_recv()
    rcopy(kv_ref.at[c], kv_ref.at[1 - c], psend.at[2], precv.at[2], partner).wait_recv()
    for d in range(2):
        for t in range(2):
            rcopy(q_ref.at[own], q_ref.at[2 * near[1 - d] + t], ssem.at[d, t], rsem.at[d, t], partner).wait_recv()
    for cp in caches:
        cp.wait()


def stage_q(qs, q_ref, first, last, chunk, hd):
    per = q_ref.shape[2] // hd
    heads = q_ref.shape[0] * per
    for t in range(first, last):
        for h in range(heads):
            to = ((t - first) * heads + h) * chunk
            for z in range(hd // LANES):
                lo = (h % per) * hd + z * LANES
                qs[z, to:to + chunk, :] = q_ref[h // per, t * chunk:(t + 1) * chunk, lo:lo + LANES].astype(F32)


def attend(qs, kb, vb, vl, acc, b0, at0, group, chunk, heads, base, scale, m_all, l_all):
    seq, hd = kb.shape[1:]
    halves = hd // LANES
    pos_iota = lax.broadcasted_iota(jnp.int32, (heads, seq), 1)
    lane_iota = lax.broadcasted_iota(jnp.int32, (heads, LANES), 1)
    scores = []
    for r in range(group):
        qb = jnp.concatenate([qs[z, pl.ds(at0 + r, heads, stride=chunk), :] for z in range(halves)], axis=1)
        scores.append(lax.dot_general(qb.astype(BF16), kb[b0 + r], (((1,), (1,)), ((), ())),
                                      preferred_element_type=F32))
    probs = []
    for r in range(group):
        valid = pos_iota < vl[b0 + r] - base
        s = jnp.where(valid, scores[r] * scale, NEG)
        m = jnp.max(s, axis=1, keepdims=True)
        p = jnp.where(valid, jnp.exp(s - m), 0.0)
        l = jnp.sum(p, axis=1, keepdims=True)
        here = lane_iota == b0 + r
        m_all = jnp.where(here, m, m_all)
        l_all = jnp.where(here, l, l_all)
        probs.append(p.astype(BF16))
    for r in range(group):
        o = jnp.dot(probs[r], vb[b0 + r], preferred_element_type=F32)
        for z in range(halves):
            acc[z, pl.ds(at0 + r, heads, stride=chunk), :] = o[:, z * LANES:(z + 1) * LANES]
    return m_all, l_all


def attend_rows(qs, kb, vb, vl, acc, first, last, group, chunk, heads, base, scale):
    def step(g, carry):
        i0 = g * group
        at0 = (i0 // chunk) * (heads * chunk) + lax.rem(i0, chunk)
        return attend(qs, kb, vb, vl, acc, first * chunk + i0, at0, group, chunk, heads, base, scale, *carry)

    init = (jnp.full((heads, LANES), NEG, F32), jnp.zeros((heads, LANES), F32))
    return lax.fori_loop(0, (last - first) * chunk // group, step, init)


def attn_kernel(group, chunk, early, scale, wp, vl, q_ref, kv_ref, k_in, v_in, ko_hbm, vo_hbm, kb, vb, acc_ref,
                ml_ref, qs, osem):
    del k_in, v_in
    rows, seq, hd = kb.shape
    heads = q_ref.shape[0] * (q_ref.shape[2] // hd)
    per = heads // ml_ref.shape[0]
    steps = rows // group
    base = lax.axis_index('sp') * seq

    def store(g):
        s = pl.ds(g * group, group)
        return (pltpu.make_async_copy(kb.at[s], ko_hbm.at[s], osem.at[0, g]),
                pltpu.make_async_copy(vb.at[s], vo_hbm.at[s], osem.at[1, g]))

    row_iota = lax.broadcasted_iota(jnp.int32, (16, hd), 0)

    def update(g, carry):
        slabs = []
        for r in range(group):
            b = g * group + r
            pos = wp[b] - base
            start = pl.multiple_of((jnp.clip(pos, 0, seq - 1) // 16) * 16, 16)
            for i, buf in enumerate((kb, vb)):
                row = jnp.broadcast_to(kv_ref[i, pl.ds(b, 1), :], (16, hd))
                slab = buf[b, pl.ds(start, 16), :].astype(F32)
                slabs.append((buf, b, start, jnp.where(row_iota == pos - start, row, slab).astype(BF16)))
        for buf, b, start, slab in slabs:
            buf[b, pl.ds(start, 16), :] = slab
        for cp in store(g):
            cp.start()
        return carry

    lax.fori_loop(0, steps, update, 0)
    stage_q(qs, q_ref, 0, early, chunk, hd)
    m_all, l_all = attend_rows(qs, kb, vb, vl, acc_ref, 0, early, group, chunk, heads, base, scale)
    for i in range(ml_ref.shape[0]):
        ml_ref[i, 0:per, :] = m_all[i * per:(i + 1) * per]
        ml_ref[i, per:2 * per, :] = l_all[i * per:(i + 1) * per]
    for g in range(steps):
        for cp in store(g):
            cp.wait()


def out_kernel(n, group, scale, vl, q_ref, kb, vb, acc_ref, ml_in, w_hbm, out_ref, qs, acc_own, ml_ref, wv,
               ra, rml, ca, sb, sml, rb, rbml, cb, sd, rd, se, re,
               wsem, amsend, amrecv, bmsend, bmrecv, asend, arecv, bsend, brecv, dsend, drecv, esend, erecv,
               fsend, frecv, gsend, grecv):
    nx = n // 2
    me = lax.axis_index('sp')
    x, c = me // 2, lax.rem(me, 2)
    partner = 2 * x + 1 - c
    wide = out_ref.shape[1] // n
    halves = acc_ref.shape[0]
    chunks, blk = ra.shape[0], ra.shape[3]
    chunk = out_ref.shape[0] // chunks
    per = blk // chunk
    heads = per * n
    early = acc_ref.shape[1] // (heads * chunk)
    far = [2, 1, 3] if nx == 4 else list(range(1, nx))
    near = [1, 3, 2] if nx == 4 else list(range(1, nx))
    order = far + [0]

    def chip(d):
        return lax.rem(x + d, nx)

    bar = pltpu.get_barrier_semaphore()
    peers = [2 * chip(d) + c for d in range(1, nx)] + [partner]
    for peer in peers:
        pl.semaphore_signal(bar, inc=1, device_id=sp_dev(peer), device_id_type=MESH)
    wloads = []
    for j in range(n):
        cp = pltpu.make_async_copy(w_hbm.at[:, j * wide:(j + 1) * wide], wv.at[j], wsem.at[j])
        cp.start()
        wloads.append(cp)
    stage_q(qs, q_ref, early, chunks, chunk, kb.shape[2])
    m_all, l_all = attend_rows(qs, kb, vb, vl, acc_own, early, chunks, group, chunk, heads, me * kb.shape[1], scale)
    late = lax.broadcasted_iota(jnp.int32, (per, LANES), 1) >= early * chunk
    for i in range(n):
        for k, u in enumerate((m_all, l_all)):
            r = slice(k * per, (k + 1) * per)
            ml_ref[i, r, :] = jnp.where(late, u[i * per:(i + 1) * per], ml_in[i, r, :])
    pl.semaphore_wait(bar, len(peers))

    def acc_at(t, j):
        if t < early:
            return acc_ref, pl.multiple_of((t * n + j) * blk, blk)
        return acc_own, pl.multiple_of(((t - early) * n + j) * blk, blk)

    pending = []

    def go(*args):
        cp = rcopy(*args)
        cp.start()
        pending.append(cp)

    def landed(*args):
        rcopy(*args, partner).wait_recv()

    for d in order:
        go(ml_ref.at[2 * chip(d) + 1 - c], rml.at[d], amsend.at[d], amrecv.at[d], partner)
    for t in range(chunks):
        for d in order:
            src, at = acc_at(t, 2 * chip(d) + 1 - c)
            go(src.at[:, pl.ds(at, blk)], ra.at[t, d], asend.at[t, d], arecv.at[t, d], partner)
    for d in order:
        landed(ml_ref.at[0], rml.at[d], amsend.at[d], amrecv.at[d])
    for d in order:
        mine, theirs = ml_ref[2 * chip(d) + c], rml[d]
        m = jnp.maximum(mine[0:per], theirs[0:per])
        fa, fb = jnp.exp(mine[0:per] - m), jnp.exp(theirs[0:per] - m)
        l = fa * mine[per:2 * per] + fb * theirs[per:2 * per]
        ca[d] = jnp.transpose(jnp.concatenate([fa, fb, m, l], axis=0))
        sml[d, 0:per, :] = m
        sml[d, per:2 * per, :] = l
    for d in far:
        go(sml.at[d], rbml.at[d], bmsend.at[d], bmrecv.at[d], 2 * chip(d) + c)

    def pair(t):
        for d in order:
            landed(ra.at[t, d], ra.at[t, d], asend.at[t, d], arecv.at[t, d])
        for d in order:
            src, at = acc_at(t, 2 * chip(d) + c)
            f = ca[d, t * chunk:(t + 1) * chunk, :]
            for h in range(per):
                r = slice(h * chunk, (h + 1) * chunk)
                for z in range(halves):
                    own = src[z, pl.ds(at + h * chunk, chunk), :]
                    sb[t, d, z, r, :] = own * f[:, h:h + 1] + ra[t, d, z, r, :] * f[:, per + h:per + h + 1]
        for d in far:
            go(sb.at[t, d], rb.at[t, d], bsend.at[t, d], brecv.at[t, d], 2 * chip(d) + c)

    for t in range(chunks):
        pair(t)
    for d in range(1, nx):
        landed(sml.at[d], rbml.at[d], bmsend.at[d], bmrecv.at[d])
    mls = [sml[0]] + [rbml[d] for d in range(1, nx)]
    m = functools.reduce(jnp.maximum, [u[0:per] for u in mls])
    fs = [jnp.exp(u[0:per] - m) for u in mls]
    l = sum(f * u[per:2 * per] for f, u in zip(fs, mls))
    cb[...] = jnp.transpose(jnp.concatenate([f / l for f in fs], axis=0))
    for cp in wloads:
        cp.wait()

    def out_at(t, j):
        return out_ref.at[pl.ds(t * chunk, chunk), pl.ds(pl.multiple_of(j * wide, wide), wide)]

    def project(t):
        for d in range(1, nx):
            landed(sb.at[t, d], rb.at[t, d], bsend.at[t, d], brecv.at[t, d])
        f = cb[t * chunk:(t + 1) * chunk, :]
        parts = []
        for h in range(per):
            r = slice(h * chunk, (h + 1) * chunk)
            for z in range(halves):
                terms = [sb[t, 0, z, r, :]] + [rb[t, d, z, r, :] for d in range(1, nx)]
                parts.append(sum(u * f[:, d * per + h:d * per + h + 1] for d, u in enumerate(terms)))
        attn = jnp.concatenate(parts, axis=1).astype(BF16)
        for d in order:
            sd[t, d] = jnp.dot(attn, wv[2 * chip(d) + 1 - c], preferred_element_type=F32)
        for d in order:
            go(sd.at[t, d], rd.at[t, d], dsend.at[t, d], drecv.at[t, d], partner)
        for d in order:
            se[t, d] = jnp.dot(attn, wv[2 * chip(d) + c], preferred_element_type=F32)

    def reduce(t):
        for d in order:
            landed(sd.at[t, d], rd.at[t, d], dsend.at[t, d], drecv.at[t, d])
        for d in order:
            se[t, d] = se[t, d] + rd[t, d]
        for d in far:
            go(se.at[t, d], re.at[t, d], esend.at[t, d], erecv.at[t, d], 2 * chip(d) + c)

    def finish(t):
        for d in range(1, nx):
            landed(se.at[t, d], re.at[t, d], esend.at[t, d], erecv.at[t, d])
        out_ref[t * chunk:(t + 1) * chunk, pl.ds(pl.multiple_of(me * wide, wide), wide)] = (
            se[t, 0] + sum(re[t, d] for d in range(1, nx))).astype(BF16)
        for d in far:
            go(out_at(t, me), out_at(t, me), fsend.at[t, d], frecv.at[t, d], 2 * chip(d) + c)
        go(out_at(t, me), out_at(t, me), gsend.at[t, 0], grecv.at[t, 0], partner)

    def forward(t):
        for d in near:
            src = 2 * chip(nx - d) + c
            landed(out_at(t, me), out_at(t, src), fsend.at[t, d], frecv.at[t, d])
            go(out_at(t, src), out_at(t, src), gsend.at[t, d], grecv.at[t, d], partner)

    project(0)
    for t in range(1, chunks):
        project(t)
        reduce(t - 1)
    reduce(chunks - 1)
    for t in range(chunks - 1):
        finish(t)
    forward(0)
    finish(chunks - 1)
    for t in range(1, chunks):
        forward(t)
    for t in range(chunks):
        for d in [0] + near:
            src = 2 * chip(nx - d if d else 0) + 1 - c
            landed(out_at(t, me), out_at(t, src), gsend.at[t, d], grecv.at[t, d])
    for cp in pending:
        cp.wait_send()


def solution(mesh):
    n = mesh.shape['sp']
    nx = n // 2
    row_spec = P(('rep', 'dp'), None)
    cache_spec = P(('rep', 'dp'), 'sp', None, None)
    len_spec = P(('rep', 'dp'))
    VM = pl.BlockSpec(memory_space=pltpu.VMEM)
    HB = pl.BlockSpec(memory_space=pltpu.HBM)
    SM = pl.BlockSpec(memory_space=pltpu.SMEM)
    DMA = pltpu.SemaphoreType.DMA

    def local_step(hidden, w_query, w_key, w_value, w_out, k_cache, v_cache, write_pos, valid_len):
        rows, seq, kv_heads, hd = k_cache.shape
        width = hidden.shape[1]
        proj = w_query.shape[1]
        heads = proj // hd
        cols = proj // n
        per = heads // n
        k3, v3 = k_cache.reshape(rows, seq, hd), v_cache.reshape(rows, seq, hd)
        sds = jax.ShapeDtypeStruct

        group, chunk = 8, rows // 4
        chunks = rows // chunk
        f = pltpu.VMEM
        q, kv, kb, vb = pl.pallas_call(
            functools.partial(qkv_kernel, n),
            out_shape=(f((n, rows, cols), BF16), f((2, rows, hd), F32),
                       f((rows, seq, hd), BF16), f((rows, seq, hd), BF16)),
            in_specs=[HB] * 6, out_specs=(VM,) * 4,
            scratch_shapes=[f((rows, width), BF16), f((2, width, cols), BF16), f((width, hd), BF16),
                            DMA, DMA((3,)), DMA((2, 4)), DMA((2, 2)), DMA((2, 2)), DMA((3,)), DMA((3,))],
            compiler_params=pltpu.CompilerParams(collective_id=0, has_side_effects=True,
                                                 vmem_limit_bytes=46 * 2 ** 20),
            name='qkv',
        )(hidden, w_query, w_key, w_value, k3, v3)

        early = chunks - 1
        halves = hd // LANES
        k_new, v_new, kb, vb, acc, ml = pl.pallas_call(
            functools.partial(attn_kernel, group, chunk, early, hd ** -0.5),
            out_shape=(sds((rows, seq, hd), BF16), sds((rows, seq, hd), BF16), f((rows, seq, hd), BF16),
                       f((rows, seq, hd), BF16), f((halves, early * heads * chunk, LANES), F32),
                       f((n, 8, LANES), F32)),
            in_specs=[SM, SM, VM, VM, VM, VM], out_specs=(HB, HB, VM, VM, VM, VM),
            scratch_shapes=[f((halves, early * heads * chunk, LANES), F32), DMA((2, rows // group))],
            input_output_aliases={4: 2, 5: 3},
            compiler_params=pltpu.CompilerParams(vmem_limit_bytes=16 * 2 ** 20),
            name='attn',
        )(write_pos, valid_len, q, kv, kb, vb)

        wide = width // n
        pair = (chunks, nx, halves, per * chunk, LANES)
        sums = (chunks, nx, chunk, wide)
        mls = (nx, 8, LANES)
        own = (halves, (chunks - early) * heads * chunk, LANES)
        out = pl.pallas_call(
            functools.partial(out_kernel, n, group, hd ** -0.5),
            out_shape=sds((rows, width), BF16),
            in_specs=[SM, VM, VM, VM, VM, VM, HB], out_specs=VM,
            scratch_shapes=[f(own, F32), f(own, F32), f((n, 8, LANES), F32), f((n, w_out.shape[0], wide), BF16),
                            f(pair, F32), f(mls, F32), f((nx, LANES, 8), F32), f(pair, F32), f(mls, F32),
                            f(pair, F32), f(mls, F32), f((LANES, 8), F32),
                            f(sums, F32), f(sums, F32), f(sums, F32), f(sums, F32),
                            DMA((n,))] + [DMA((nx,))] * 4 + [DMA((chunks, nx))] * 12,
            compiler_params=pltpu.CompilerParams(collective_id=1, has_side_effects=True,
                                                 vmem_limit_bytes=20 * 2 ** 20),
            name='outp',
        )(valid_len, q, kb, vb, acc, ml, pltpu.with_memory_space_constraint(w_out, pltpu.HBM))
        return out, k_new.reshape(k_cache.shape), v_new.reshape(v_cache.shape)

    return jax.shard_map(local_step, mesh=mesh,
                         in_specs=(row_spec, P(), P(), P(), P('sp', None), cache_spec, cache_spec, len_spec, len_spec),
                         out_specs=(row_spec, cache_spec, cache_spec), check_vma=False)
```

```python
import functools

import jax
import jax.numpy as jnp
from jax import lax
from jax.experimental import pallas as pl
from jax.experimental.pallas import tpu as pltpu
from jax.sharding import PartitionSpec as P

MESH = pl.DeviceIdType.MESH
NEG = -3.4e38
LANES = 128
F32 = jnp.float32
BF16 = jnp.bfloat16


def sp_dev(i):
    return {'sp': i}


def rcopy(src, dst, ss, rs, dev):
    return pltpu.make_async_remote_copy(src_ref=src, dst_ref=dst, send_sem=ss, recv_sem=rs,
                                        device_id=sp_dev(dev), device_id_type=MESH)


def qkv_kernel(n, hid_hbm, wq_hbm, wk_hbm, wv_hbm, k_hbm, v_hbm, q_ref, kv_ref, kb, vb,
               hid, wq, wkv, hsem, wsem, csem, ssem, rsem, psend, precv):
    nx = n // 2
    me = lax.axis_index('sp')
    x, c = me // 2, lax.rem(me, 2)
    cols = wq.shape[2]
    own = me
    opp = 2 * lax.rem(x + nx // 2, nx) + c
    partner = 2 * x + 1 - c
    ch = pltpu.make_async_copy(hid_hbm, hid, hsem)
    ch.start()
    loads = []
    for i, blk in enumerate((own, opp)):
        cp = pltpu.make_async_copy(wq_hbm.at[:, pl.ds(pl.multiple_of(blk * cols, cols), cols)], wq.at[i], wsem.at[i])
        cp.start()
        loads.append(cp)
    near = [lax.rem(x + d, nx) for d in (1, nx - 1)]
    bar = pltpu.get_barrier_semaphore()
    peers = [2 * t + u for t in near for u in range(2)] + [partner]
    for peer in peers:
        pl.semaphore_signal(bar, inc=1, device_id=sp_dev(peer), device_id_type=MESH)
    pick = [pltpu.make_async_copy(w, wkv, wsem.at[2]) for w in (wk_hbm, wv_hbm)]
    for i in range(2):
        @pl.when(c == i)
        def _():
            pick[i].start()
    ch.wait()
    loads[0].wait()
    parts = csem.shape[1]
    step = kb.shape[0] // parts
    caches = []
    for g in range(parts):
        for i, (src, dst) in enumerate(((k_hbm, kb), (v_hbm, vb))):
            cp = pltpu.make_async_copy(src.at[pl.ds(g * step, step)], dst.at[pl.ds(g * step, step)], csem.at[i, g])
            cp.start()
            caches.append(cp)

    def project(w):
        return jnp.dot(hid[...], w, preferred_element_type=F32).astype(BF16)

    q_ref[own] = project(wq[0])
    pl.semaphore_wait(bar, len(peers))
    sends = []
    for d in range(2):
        for t in range(2):
            sends.append(rcopy(q_ref.at[own], q_ref.at[own], ssem.at[d, t], rsem.at[d, c], 2 * near[d] + t))
    sends.append(rcopy(q_ref.at[own], q_ref.at[own], psend.at[0], precv.at[0], partner))
    for s in sends:
        s.start()
    loads[1].wait()
    q_ref[opp] = project(wq[1])
    sends.append(rcopy(q_ref.at[opp], q_ref.at[opp], psend.at[1], precv.at[1], partner))
    sends[-1].start()
    pick[0].wait()
    kv_ref[c] = project(wkv[...])
    sends.append(rcopy(kv_ref.at[c], kv_ref.at[c], psend.at[2], precv.at[2], partner))
    sends[-1].start()
    for s in sends:
        s.wait_send()
    popp = 2 * lax.rem(x + nx // 2, nx) + 1 - c
    rcopy(q_ref.at[own], q_ref.at[partner], psend.at[0], precv.at[0], partner).wait_recv()
    rcopy(q_ref.at[own], q_ref.at[popp], psend.at[1], precv.at[1], partner).wait_recv()
    rcopy(kv_ref.at[c], kv_ref.at[1 - c], psend.at[2], precv.at[2], partner).wait_recv()
    for d in range(2):
        for t in range(2):
            rcopy(q_ref.at[own], q_ref.at[2 * near[1 - d] + t], ssem.at[d, t], rsem.at[d, t], partner).wait_recv()
    for cp in caches:
        cp.wait()


def stage_q(qs, q_ref, t, chunk, hd):
    per = q_ref.shape[2] // hd
    for h in range(q_ref.shape[0] * per):
        for z in range(hd // LANES):
            lo = (h % per) * hd + z * LANES
            qs[z, h * chunk:(h + 1) * chunk, :] = q_ref[h // per, t * chunk:(t + 1) * chunk, lo:lo + LANES].astype(F32)


def attend(qs, kb, vb, vl, acc, b0, at0, group, chunk, heads, base, scale, m_all, l_all):
    seq, hd = kb.shape[1:]
    halves = hd // LANES
    pos_iota = lax.broadcasted_iota(jnp.int32, (heads, seq), 1)
    lane_iota = lax.broadcasted_iota(jnp.int32, (heads, LANES), 1)
    scores = []
    for r in range(group):
        qb = jnp.concatenate([qs[z, pl.ds(at0 + r, heads, stride=chunk), :] for z in range(halves)], axis=1)
        scores.append(lax.dot_general(qb.astype(BF16), kb[b0 + at0 + r], (((1,), (1,)), ((), ())),
                                      preferred_element_type=F32))
    probs = []
    for r in range(group):
        valid = pos_iota < vl[b0 + at0 + r] - base
        s = jnp.where(valid, scores[r] * scale, NEG)
        m = jnp.max(s, axis=1, keepdims=True)
        p = jnp.where(valid, jnp.exp(s - m), 0.0)
        l = jnp.sum(p, axis=1, keepdims=True)
        here = lane_iota == at0 + r
        m_all = jnp.where(here, m, m_all)
        l_all = jnp.where(here, l, l_all)
        probs.append(p.astype(BF16))
    for r in range(group):
        o = jnp.dot(probs[r], vb[b0 + at0 + r], preferred_element_type=F32)
        for z in range(halves):
            acc[z, pl.ds(at0 + r, heads, stride=chunk), :] = o[:, z * LANES:(z + 1) * LANES]
    return m_all, l_all


def attn_out_kernel(n, group, scale, vl, q_ref, kb, vb, w_hbm, out_ref, qs, acc, ml, wv,
                    ra, rml, sb, sml, rb, rbml, sd, rd, se, re,
                    wsem, amsend, amrecv, bmsend, bmrecv, asend, arecv, bsend, brecv, dsend, drecv, esend, erecv,
                    fsend, frecv, gsend, grecv):
    nx = n // 2
    me = lax.axis_index('sp')
    x, c = me // 2, lax.rem(me, 2)
    partner = 2 * x + 1 - c
    wide = out_ref.shape[1] // n
    chunks, halves = acc.shape[:2]
    blk = acc.shape[2] // n
    chunk = out_ref.shape[0] // chunks
    per = blk // chunk
    heads = per * n
    hd = kb.shape[2]
    far = [2, 1, 3] if nx == 4 else list(range(1, nx))
    near = [1, 3, 2] if nx == 4 else list(range(1, nx))
    order = far + [0]

    def chip(d):
        return lax.rem(x + d, nx)

    bar = pltpu.get_barrier_semaphore()
    peers = [2 * chip(d) + c for d in range(1, nx)] + [partner]
    for peer in peers:
        pl.semaphore_signal(bar, inc=1, device_id=sp_dev(peer), device_id_type=MESH)
    wloads = []
    for j in range(n):
        cp = pltpu.make_async_copy(w_hbm.at[:, j * wide:(j + 1) * wide], wv.at[j], wsem.at[j])
        cp.start()
        wloads.append(cp)

    pending = []

    def go(*args):
        cp = rcopy(*args)
        cp.start()
        pending.append(cp)

    def landed(*args):
        rcopy(*args, partner).wait_recv()

    def acc_at(j):
        return pl.multiple_of(j * blk, blk)

    def local(t):
        stage_q(qs.at[t], q_ref, t, chunk, hd)

        def step(g, carry):
            return attend(qs.at[t], kb, vb, vl, acc.at[t], t * chunk, g * group, group, chunk, heads,
                          me * kb.shape[1], scale, *carry)

        init = (jnp.full((heads, LANES), NEG, F32), jnp.zeros((heads, LANES), F32))
        m_all, l_all = lax.fori_loop(0, chunk // group, step, init)
        for i in range(n):
            ml[t, i, 0:per, :] = m_all[i * per:(i + 1) * per]
            ml[t, i, per:2 * per, :] = l_all[i * per:(i + 1) * per]

    def share(t):
        for d in order:
            j = 2 * chip(d) + 1 - c
            go(ml.at[t, j], rml.at[t, d], amsend.at[t, d], amrecv.at[t, d], partner)
            go(acc.at[t, :, pl.ds(acc_at(j), blk)], ra.at[t, d], asend.at[t, d], arecv.at[t, d], partner)

    def pair(t):
        for d in order:
            landed(ml.at[t, 0], rml.at[t, d], amsend.at[t, d], amrecv.at[t, d])
            landed(ra.at[t, d], ra.at[t, d], asend.at[t, d], arecv.at[t, d])
        for d in order:
            j = 2 * chip(d) + c
            mine, theirs = ml[t, j], rml[t, d]
            m = jnp.maximum(mine[0:per], theirs[0:per])
            fa, fb = jnp.exp(mine[0:per] - m), jnp.exp(theirs[0:per] - m)
            l = fa * mine[per:2 * per] + fb * theirs[per:2 * per]
            f = jnp.transpose(jnp.concatenate([fa, fb, m, l], axis=0))[0:chunk]
            sml[t, d, 0:per, :] = m
            sml[t, d, per:2 * per, :] = l
            for h in range(per):
                r = slice(h * chunk, (h + 1) * chunk)
                for z in range(halves):
                    own = acc[t, z, pl.ds(acc_at(j) + h * chunk, chunk), :]
                    sb[t, d, z, r, :] = own * f[:, h:h + 1] + ra[t, d, z, r, :] * f[:, per + h:per + h + 1]
        for d in far:
            j = 2 * chip(d) + c
            go(sml.at[t, d], rbml.at[t, d], bmsend.at[t, d], bmrecv.at[t, d], j)
            go(sb.at[t, d], rb.at[t, d], bsend.at[t, d], brecv.at[t, d], j)

    def out_at(t, j):
        return out_ref.at[pl.ds(t * chunk, chunk), pl.ds(pl.multiple_of(j * wide, wide), wide)]

    def project(t):
        for d in range(1, nx):
            landed(sml.at[t, d], rbml.at[t, d], bmsend.at[t, d], bmrecv.at[t, d])
            landed(sb.at[t, d], rb.at[t, d], bsend.at[t, d], brecv.at[t, d])
        mls = [sml[t, 0]] + [rbml[t, d] for d in range(1, nx)]
        m = functools.reduce(jnp.maximum, [u[0:per] for u in mls])
        fs = [jnp.exp(u[0:per] - m) for u in mls]
        l = sum(f * u[per:2 * per] for f, u in zip(fs, mls))
        f = jnp.transpose(jnp.concatenate([f / l for f in fs], axis=0))[0:chunk]
        parts = []
        for h in range(per):
            r = slice(h * chunk, (h + 1) * chunk)
            for z in range(halves):
                terms = [sb[t, 0, z, r, :]] + [rb[t, d, z, r, :] for d in range(1, nx)]
                parts.append(sum(u * f[:, d * per + h:d * per + h + 1] for d, u in enumerate(terms)))
        attn = jnp.concatenate(parts, axis=1).astype(BF16)
        for d in order:
            sd[t, d] = jnp.dot(attn, wv[2 * chip(d) + 1 - c], preferred_element_type=F32)
        for d in order:
            go(sd.at[t, d], rd.at[t, d], dsend.at[t, d], drecv.at[t, d], partner)
        for d in order:
            se[t, d] = jnp.dot(attn, wv[2 * chip(d) + c], preferred_element_type=F32)

    def reduce(t):
        for d in order:
            landed(sd.at[t, d], rd.at[t, d], dsend.at[t, d], drecv.at[t, d])
        for d in order:
            se[t, d] = se[t, d] + rd[t, d]
        for d in far:
            go(se.at[t, d], re.at[t, d], esend.at[t, d], erecv.at[t, d], 2 * chip(d) + c)

    def finish(t):
        for d in range(1, nx):
            landed(se.at[t, d], re.at[t, d], esend.at[t, d], erecv.at[t, d])
        out_ref[t * chunk:(t + 1) * chunk, pl.ds(pl.multiple_of(me * wide, wide), wide)] = (
            se[t, 0] + sum(re[t, d] for d in range(1, nx))).astype(BF16)
        for d in far:
            go(out_at(t, me), out_at(t, me), fsend.at[t, d], frecv.at[t, d], 2 * chip(d) + c)
        go(out_at(t, me), out_at(t, me), gsend.at[t, 0], grecv.at[t, 0], partner)

    def forward(t):
        for d in near:
            src = 2 * chip(nx - d) + c
            landed(out_at(t, me), out_at(t, src), fsend.at[t, d], frecv.at[t, d])
            go(out_at(t, src), out_at(t, src), gsend.at[t, d], grecv.at[t, d], partner)

    local(0)
    pl.semaphore_wait(bar, len(peers))
    share(0)
    for t in range(1, chunks):
        local(t)
        share(t)
        pair(t - 1)
    for cp in wloads:
        cp.wait()
    project(0)
    pair(chunks - 1)
    for t in range(1, chunks):
        project(t)
        reduce(t - 1)
    reduce(chunks - 1)
    for t in range(chunks - 1):
        finish(t)
    forward(0)
    finish(chunks - 1)
    for t in range(1, chunks):
        forward(t)
    for t in range(chunks):
        for d in [0] + near:
            src = 2 * chip(nx - d if d else 0) + 1 - c
            landed(out_at(t, me), out_at(t, src), gsend.at[t, d], grecv.at[t, d])
    for cp in pending:
        cp.wait_send()


def solution(mesh):
    n = mesh.shape['sp']
    nx = n // 2
    row_spec = P(('rep', 'dp'), None)
    cache_spec = P(('rep', 'dp'), 'sp', None, None)
    len_spec = P(('rep', 'dp'))
    VM = pl.BlockSpec(memory_space=pltpu.VMEM)
    HB = pl.BlockSpec(memory_space=pltpu.HBM)
    SM = pl.BlockSpec(memory_space=pltpu.SMEM)
    DMA = pltpu.SemaphoreType.DMA

    def local_step(hidden, w_query, w_key, w_value, w_out, k_cache, v_cache, write_pos, valid_len):
        rows, seq, kv_heads, hd = k_cache.shape
        width = hidden.shape[1]
        proj = w_query.shape[1]
        heads = proj // hd
        cols = proj // n
        per = heads // n
        k3, v3 = k_cache.reshape(rows, seq, hd), v_cache.reshape(rows, seq, hd)
        sds = jax.ShapeDtypeStruct

        group, chunk = 8, rows // 4
        chunks = rows // chunk
        f = pltpu.VMEM
        q, kv, kb, vb = pl.pallas_call(
            functools.partial(qkv_kernel, n),
            out_shape=(f((n, rows, cols), BF16), sds((2, rows, hd), BF16),
                       f((rows, seq, hd), BF16), f((rows, seq, hd), BF16)),
            in_specs=[HB] * 6, out_specs=(VM,) * 4,
            scratch_shapes=[f((rows, width), BF16), f((2, width, cols), BF16), f((width, hd), BF16),
                            DMA, DMA((3,)), DMA((2, 4)), DMA((2, 2)), DMA((2, 2)), DMA((3,)), DMA((3,))],
            compiler_params=pltpu.CompilerParams(collective_id=0, has_side_effects=True,
                                                 vmem_limit_bytes=46 * 2 ** 20),
            name='qkv',
        )(hidden, w_query, w_key, w_value, k3, v3)

        place = lax.axis_index('sp') * seq + jnp.arange(seq, dtype=jnp.int32)
        at_pos = (place[None, :] == write_pos[:, None])[:, :, None]
        k_new = jnp.where(at_pos, kv[0][:, None, :], kb)
        v_new = jnp.where(at_pos, kv[1][:, None, :], vb)

        halves = hd // LANES
        wide = width // n
        pair = (chunks, nx, halves, per * chunk, LANES)
        sums = (chunks, nx, chunk, wide)
        mls = (chunks, nx, 8, LANES)
        own = (chunks, halves, heads * chunk, LANES)
        out = pl.pallas_call(
            functools.partial(attn_out_kernel, n, group, hd ** -0.5),
            out_shape=sds((rows, width), BF16),
            in_specs=[SM, VM, VM, VM, HB], out_specs=VM,
            scratch_shapes=[f(own, F32), f(own, F32), f((chunks, n, 8, LANES), F32),
                            f((n, w_out.shape[0], wide), BF16),
                            f(pair, F32), f(mls, F32), f(pair, F32), f(mls, F32), f(pair, F32), f(mls, F32),
                            f(sums, F32), f(sums, F32), f(sums, F32), f(sums, F32),
                            DMA((n,))] + [DMA((chunks, nx))] * 16,
            cost_estimate=pl.CostEstimate(flops=30 * 10 ** 9, bytes_accessed=60 * 10 ** 6, transcendentals=0),
            compiler_params=pltpu.CompilerParams(collective_id=1, has_side_effects=True,
                                                 vmem_limit_bytes=20 * 2 ** 20),
            name='attn_out',
        )(valid_len, q, k_new, v_new, pltpu.with_memory_space_constraint(w_out, pltpu.HBM))
        return out, k_new.reshape(k_cache.shape), v_new.reshape(v_cache.shape)

    return jax.shard_map(local_step, mesh=mesh,
                         in_specs=(row_spec, P(), P(), P(), P('sp', None), cache_spec, cache_spec, len_spec, len_spec),
                         out_specs=(row_spec, cache_spec, cache_spec), check_vma=False)
```

```python
import functools

import jax
import jax.numpy as jnp
from jax import lax
from jax.experimental import pallas as pl
from jax.experimental.pallas import tpu as pltpu
from jax.sharding import PartitionSpec as P

MESH = pl.DeviceIdType.MESH
NEG = -3.4e38
LANES = 128
F32 = jnp.float32
BF16 = jnp.bfloat16


def sp_dev(i):
    return {'sp': i}


def rcopy(src, dst, ss, rs, dev):
    return pltpu.make_async_remote_copy(src_ref=src, dst_ref=dst, send_sem=ss, recv_sem=rs,
                                        device_id=sp_dev(dev), device_id_type=MESH)


def qkv_kernel(n, group, chunk, scale, hid_hbm, wq_hbm, wk_hbm, wv_hbm, k_hbm, v_hbm, wp_hbm, vl_hbm,
               q_ref, kv_ref, kb, vb, acc, ml, hid, wq, wkv, qs, kvs, wp, vl, hsem, wsem, csem, isem, ssem, rsem, psend,
               precv):
    nx = n // 2
    me = lax.axis_index('sp')
    x, c = me // 2, lax.rem(me, 2)
    cols = wq.shape[2]
    own = me
    opp = 2 * lax.rem(x + nx // 2, nx) + c
    partner = 2 * x + 1 - c
    ch = pltpu.make_async_copy(hid_hbm, hid, hsem)
    ch.start()
    loads = []
    for i, blk in enumerate((own, opp)):
        cp = pltpu.make_async_copy(wq_hbm.at[:, pl.ds(pl.multiple_of(blk * cols, cols), cols)], wq.at[i], wsem.at[i])
        cp.start()
        loads.append(cp)
    ints = [pltpu.make_async_copy(src, dst, isem.at[i]) for i, (src, dst) in enumerate(((wp_hbm, wp), (vl_hbm, vl)))]
    for cp in ints:
        cp.start()
    near = [lax.rem(x + d, nx) for d in (1, nx - 1)]
    bar = pltpu.get_barrier_semaphore()
    peers = [2 * t + u for t in near for u in range(2)] + [partner]
    for peer in peers:
        pl.semaphore_signal(bar, inc=1, device_id=sp_dev(peer), device_id_type=MESH)
    pick = [pltpu.make_async_copy(w, wkv, wsem.at[2]) for w in (wk_hbm, wv_hbm)]
    for i in range(2):
        @pl.when(c == i)
        def _():
            pick[i].start()
    ch.wait()
    loads[0].wait()
    parts = csem.shape[1]
    step = kb.shape[0] // parts
    caches = []
    for g in range(parts):
        for i, (src, dst) in enumerate(((k_hbm, kb), (v_hbm, vb))):
            cp = pltpu.make_async_copy(src.at[pl.ds(g * step, step)], dst.at[pl.ds(g * step, step)], csem.at[i, g])
            cp.start()
            caches.append(cp)

    def project(w):
        return jnp.dot(hid[...], w, preferred_element_type=F32).astype(BF16)

    q_ref[own] = project(wq[0])
    pl.semaphore_wait(bar, len(peers))
    sends = []
    for d in range(2):
        for t in range(2):
            sends.append(rcopy(q_ref.at[own], q_ref.at[own], ssem.at[d, t], rsem.at[d, c], 2 * near[d] + t))
    sends.append(rcopy(q_ref.at[own], q_ref.at[own], psend.at[0], precv.at[0], partner))
    for s in sends:
        s.start()
    loads[1].wait()
    q_ref[opp] = project(wq[1])
    sends.append(rcopy(q_ref.at[opp], q_ref.at[opp], psend.at[1], precv.at[1], partner))
    sends[-1].start()
    pick[0].wait()
    kv_ref[c] = project(wkv[...])
    sends.append(rcopy(kv_ref.at[c], kv_ref.at[c], psend.at[2], precv.at[2], partner))
    sends[-1].start()
    for s in sends:
        s.wait_send()
    popp = 2 * lax.rem(x + nx // 2, nx) + 1 - c
    rcopy(q_ref.at[own], q_ref.at[partner], psend.at[0], precv.at[0], partner).wait_recv()
    rcopy(q_ref.at[own], q_ref.at[popp], psend.at[1], precv.at[1], partner).wait_recv()
    rcopy(kv_ref.at[c], kv_ref.at[1 - c], psend.at[2], precv.at[2], partner).wait_recv()
    for d in range(2):
        for t in range(2):
            rcopy(q_ref.at[own], q_ref.at[2 * near[1 - d] + t], ssem.at[d, t], rsem.at[d, t], partner).wait_recv()
    for cp in ints + caches[:2]:
        cp.wait()
    kvs[...] = kv_ref[:, 0:chunk, :].astype(F32)
    attend_chunk(qs, q_ref, kb, vb, vl, acc, ml, 0, group, chunk, me * kb.shape[1], scale, (wp, kvs))
    for cp in caches[2:]:
        cp.wait()


def stage_q(qs, q_ref, t, chunk, hd):
    per = q_ref.shape[2] // hd
    for h in range(q_ref.shape[0] * per):
        for z in range(hd // LANES):
            lo = (h % per) * hd + z * LANES
            qs[z, h * chunk:(h + 1) * chunk, :] = q_ref[h // per, t * chunk:(t + 1) * chunk, lo:lo + LANES].astype(F32)


def attend(qs, kb, vb, vl, acc, b0, at0, group, chunk, heads, base, scale, m_all, l_all, fresh=None):
    seq, hd = kb.shape[1:]
    halves = hd // LANES
    pos_iota = lax.broadcasted_iota(jnp.int32, (heads, seq), 1)
    lane_iota = lax.broadcasted_iota(jnp.int32, (heads, LANES), 1)
    scores = []
    for r in range(group):
        qb = jnp.concatenate([qs[z, pl.ds(at0 + r, heads, stride=chunk), :] for z in range(halves)], axis=1)
        scores.append(lax.dot_general(qb.astype(BF16), kb[b0 + at0 + r], (((1,), (1,)), ((), ())),
                                      preferred_element_type=F32))
    probs, extra = [], []
    for r in range(group):
        valid = pos_iota < vl[b0 + at0 + r] - base
        s = scores[r]
        if fresh is not None:
            wp, kvs = fresh
            newest = pos_iota == wp[b0 + at0 + r] - base
            qb = jnp.concatenate([qs[z, pl.ds(at0 + r, heads, stride=chunk), :] for z in range(halves)], axis=1)
            s = jnp.where(newest, jnp.sum(qb * kvs[0, pl.ds(at0 + r, 1), :], axis=1, keepdims=True), s)
        s = jnp.where(valid, s * scale, NEG)
        m = jnp.max(s, axis=1, keepdims=True)
        p = jnp.where(valid, jnp.exp(s - m), 0.0)
        l = jnp.sum(p, axis=1, keepdims=True)
        here = lane_iota == at0 + r
        m_all = jnp.where(here, m, m_all)
        l_all = jnp.where(here, l, l_all)
        p = p.astype(BF16)
        if fresh is not None:
            p = p.astype(F32)
            extra.append(jnp.sum(jnp.where(newest, p, 0.0), axis=1, keepdims=True) * kvs[1, pl.ds(at0 + r, 1), :])
            p = jnp.where(newest, 0.0, p).astype(BF16)
        probs.append(p)
    for r in range(group):
        o = jnp.dot(probs[r], vb[b0 + at0 + r], preferred_element_type=F32)
        if fresh is not None:
            o = o + extra[r]
        for z in range(halves):
            acc[z, pl.ds(at0 + r, heads, stride=chunk), :] = o[:, z * LANES:(z + 1) * LANES]
    return m_all, l_all


def attend_chunk(qs, q_ref, kb, vb, vl, acc, ml, t, group, chunk, base, scale, fresh=None):
    n, hd = q_ref.shape[0], kb.shape[2]
    per = q_ref.shape[2] // hd
    heads = n * per
    stage_q(qs, q_ref, t, chunk, hd)

    def step(g, carry):
        return attend(qs, kb, vb, vl, acc, t * chunk, g * group, group, chunk, heads, base, scale, *carry, fresh)

    init = (jnp.full((heads, LANES), NEG, F32), jnp.zeros((heads, LANES), F32))
    m_all, l_all = lax.fori_loop(0, chunk // group, step, init)
    for i in range(n):
        ml[i, 0:per, :] = m_all[i * per:(i + 1) * per]
        ml[i, per:2 * per, :] = l_all[i * per:(i + 1) * per]


def attn_out_kernel(n, group, scale, vl_hbm, q_ref, kb, vb, acc0, ml0, w_ref, out_ref, qs, acc, ml, vl, vsem,
                    ra, rml, sb, sml, rb, rbml, sd, rd, se, re,
                    amsend, amrecv, bmsend, bmrecv, asend, arecv, bsend, brecv, dsend, drecv, esend, erecv,
                    fsend, frecv, gsend, grecv):
    nx = n // 2
    me = lax.axis_index('sp')
    x, c = me // 2, lax.rem(me, 2)
    partner = 2 * x + 1 - c
    wide = out_ref.shape[1] // n
    chunks, halves = acc.shape[0] + 1, acc.shape[1]
    blk = acc.shape[2] // n
    chunk = out_ref.shape[0] // chunks
    per = blk // chunk
    heads = per * n
    hd = kb.shape[2]
    far = [2, 1, 3] if nx == 4 else list(range(1, nx))
    near = [1, 3, 2] if nx == 4 else list(range(1, nx))
    order = far + [0]

    def chip(d):
        return lax.rem(x + d, nx)

    bar = pltpu.get_barrier_semaphore()
    peers = [2 * chip(d) + u for d in range(1, nx) for u in range(2)] + [partner]
    for peer in peers:
        pl.semaphore_signal(bar, inc=1, device_id=sp_dev(peer), device_id_type=MESH)
    lens = pltpu.make_async_copy(vl_hbm, vl, vsem)
    lens.start()

    def w_at(j):
        return w_ref[:, pl.ds(pl.multiple_of(j * wide, wide), wide)]

    pending = []

    def go(*args):
        cp = rcopy(*args)
        cp.start()
        pending.append(cp)

    def landed(*args):
        rcopy(*args, partner).wait_recv()

    def acc_at(j):
        return pl.multiple_of(j * blk, blk)

    def local(t):
        attend_chunk(qs.at[t - 1], q_ref, kb, vb, vl, acc.at[t - 1], ml.at[t - 1], t, group, chunk, me * kb.shape[1], scale)

    def acc_of(t):
        return acc.at[t - 1] if t else acc0

    def ml_of(t):
        return ml.at[t - 1] if t else ml0

    def share(t):
        for d in order:
            j = 2 * chip(d) + 1 - c
            go(ml_of(t).at[j], rml.at[t, d], amsend.at[t, d], amrecv.at[t, d], partner)
            go(acc_of(t).at[:, pl.ds(acc_at(j), blk)], ra.at[t, d], asend.at[t, d], arecv.at[t, d], partner)

    def pair(t):
        for d in order:
            landed(ml_of(t).at[0], rml.at[t, d], amsend.at[t, d], amrecv.at[t, d])
            landed(ra.at[t, d], ra.at[t, d], asend.at[t, d], arecv.at[t, d])
        for d in order:
            j = 2 * chip(d) + c
            mine, theirs = ml_of(t)[j], rml[t, d]
            m = jnp.maximum(mine[0:per], theirs[0:per])
            fa, fb = jnp.exp(mine[0:per] - m), jnp.exp(theirs[0:per] - m)
            l = fa * mine[per:2 * per] + fb * theirs[per:2 * per]
            f = jnp.transpose(jnp.concatenate([fa, fb, m, l], axis=0))[0:chunk]
            sml[t, d, 0:per, :] = m
            sml[t, d, per:2 * per, :] = l
            for h in range(per):
                r = slice(h * chunk, (h + 1) * chunk)
                for z in range(halves):
                    own = acc_of(t)[z, pl.ds(acc_at(j) + h * chunk, chunk), :]
                    sb[t, d, z, r, :] = own * f[:, h:h + 1] + ra[t, d, z, r, :] * f[:, per + h:per + h + 1]
        for d in far:
            j = 2 * chip(d) + c
            go(sml.at[t, d], rbml.at[t, d], bmsend.at[t, d], bmrecv.at[t, d], j)
            go(sb.at[t, d], rb.at[t, d], bsend.at[t, d], brecv.at[t, d], j)

    def out_at(t, j):
        return out_ref.at[pl.ds(t * chunk, chunk), pl.ds(pl.multiple_of(j * wide, wide), wide)]

    def project(t):
        for d in range(1, nx):
            landed(sml.at[t, d], rbml.at[t, d], bmsend.at[t, d], bmrecv.at[t, d])
            landed(sb.at[t, d], rb.at[t, d], bsend.at[t, d], brecv.at[t, d])
        mls = [sml[t, 0]] + [rbml[t, d] for d in range(1, nx)]
        m = functools.reduce(jnp.maximum, [u[0:per] for u in mls])
        fs = [jnp.exp(u[0:per] - m) for u in mls]
        l = sum(f * u[per:2 * per] for f, u in zip(fs, mls))
        f = jnp.transpose(jnp.concatenate([f / l for f in fs], axis=0))[0:chunk]
        parts = []
        for h in range(per):
            r = slice(h * chunk, (h + 1) * chunk)
            for z in range(halves):
                terms = [sb[t, 0, z, r, :]] + [rb[t, d, z, r, :] for d in range(1, nx)]
                parts.append(sum(u * f[:, d * per + h:d * per + h + 1] for d, u in enumerate(terms)))
        attn = jnp.concatenate(parts, axis=1).astype(BF16)
        for d in order:
            sd[t, d] = jnp.dot(attn, w_at(2 * chip(d) + 1 - c), preferred_element_type=F32)
        for d in order:
            go(sd.at[t, d], rd.at[t, d], dsend.at[t, d], drecv.at[t, d], partner)
        for d in order:
            se[t, d] = jnp.dot(attn, w_at(2 * chip(d) + c), preferred_element_type=F32)

    def reduce(t):
        for d in order:
            landed(sd.at[t, d], rd.at[t, d], dsend.at[t, d], drecv.at[t, d])
        for d in order:
            se[t, d] = se[t, d] + rd[t, d]
        for d in far:
            go(se.at[t, d], re.at[t, d], esend.at[t, d], erecv.at[t, d], 2 * chip(d) + c)

    def finish(t):
        for d in range(1, nx):
            landed(se.at[t, d], re.at[t, d], esend.at[t, d], erecv.at[t, d])
        out_ref[t * chunk:(t + 1) * chunk, pl.ds(pl.multiple_of(me * wide, wide), wide)] = (
            se[t, 0] + sum(re[t, d] for d in range(1, nx))).astype(BF16)
        last = t == chunks - 1
        for d in far:
            go(out_at(t, me), out_at(t, me), fsend.at[t, d], frecv.at[t, d], 2 * chip(d) + c)
            if last:
                go(out_at(t, me), out_at(t, me), gsend.at[t, d], grecv.at[t, d], 2 * chip(d) + 1 - c)
        go(out_at(t, me), out_at(t, me), gsend.at[t, 0], grecv.at[t, 0], partner)

    def forward(t):
        for d in near:
            src = 2 * chip(nx - d) + c
            landed(out_at(t, me), out_at(t, src), fsend.at[t, d], frecv.at[t, d])
            if t < chunks - 1:
                go(out_at(t, src), out_at(t, src), gsend.at[t, d], grecv.at[t, d], partner)

    pl.semaphore_wait(bar, len(peers))
    share(0)
    lens.wait()
    local(1)
    share(1)
    pair(0)
    for t in range(2, chunks):
        local(t)
        share(t)
        pair(t - 1)
    project(0)
    pair(chunks - 1)
    reduce(0)
    for t in range(1, chunks):
        project(t)
        reduce(t)
    for t in range(chunks):
        finish(t)
    for t in range(chunks):
        forward(t)
    for t in range(chunks):
        for d in [0] + near:
            src = 2 * chip(nx - d if d else 0) + 1 - c
            landed(out_at(t, me), out_at(t, src), gsend.at[t, d], grecv.at[t, d])
    for cp in pending:
        cp.wait_send()


def solution(mesh):
    n = mesh.shape['sp']
    nx = n // 2
    row_spec = P(('rep', 'dp'), None)
    cache_spec = P(('rep', 'dp'), 'sp', None, None)
    len_spec = P(('rep', 'dp'))
    VM = pl.BlockSpec(memory_space=pltpu.VMEM)
    HB = pl.BlockSpec(memory_space=pltpu.HBM)
    SM = pl.BlockSpec(memory_space=pltpu.SMEM)
    DMA = pltpu.SemaphoreType.DMA

    def local_step(hidden, w_query, w_key, w_value, w_out, k_cache, v_cache, write_pos, valid_len):
        rows, seq, kv_heads, hd = k_cache.shape
        width = hidden.shape[1]
        proj = w_query.shape[1]
        heads = proj // hd
        cols = proj // n
        per = heads // n
        k3, v3 = k_cache.reshape(rows, seq, hd), v_cache.reshape(rows, seq, hd)
        sds = jax.ShapeDtypeStruct

        group, chunk = 8, rows // 4
        chunks = rows // chunk
        f = pltpu.VMEM
        halves = hd // LANES
        own = (halves, heads * chunk, LANES)
        hbm = [pltpu.with_memory_space_constraint(u, pltpu.HBM)
               for u in (hidden, w_query, w_key, w_value, k3, v3, write_pos, valid_len)]
        q, kv, kb, vb, acc0, ml0 = pl.pallas_call(
            functools.partial(qkv_kernel, n, group, chunk, hd ** -0.5),
            out_shape=(f((n, rows, cols), BF16), f((2, rows, hd), BF16),
                       f((rows, seq, hd), BF16), f((rows, seq, hd), BF16), f(own, F32), f((n, 2 * per, LANES), F32)),
            in_specs=[HB] * 8, out_specs=(VM,) * 6,
            scratch_shapes=[f((rows, width), BF16), f((2, width, cols), BF16), f((width, hd), BF16),
                            f(own, F32), f((2, chunk, hd), F32), pltpu.SMEM((rows,), jnp.int32),
                            pltpu.SMEM((rows,), jnp.int32),
                            DMA, DMA((3,)), DMA((2, chunks)), DMA((2,)), DMA((2, 2)), DMA((2, 2)), DMA((3,)), DMA((3,))],
            compiler_params=pltpu.CompilerParams(collective_id=0, has_side_effects=True,
                                                 vmem_limit_bytes=24 * 2 ** 20),
            name='qkv',
        )(*hbm)

        kv, when = lax.optimization_barrier((kv, write_pos))
        place = lax.axis_index('sp') * seq + jnp.arange(seq, dtype=jnp.int32)
        at_pos = (place[None, :] == when[:, None])[:, :, None]
        k_new = jnp.where(at_pos, kv[0][:, None, :], kb)
        v_new = jnp.where(at_pos, kv[1][:, None, :], vb)

        wide = width // n
        pair = (chunks, nx, halves, per * chunk, LANES)
        sums = (chunks, nx, chunk, wide)
        mls = (chunks, nx, 2 * per, LANES)
        own = (chunks - 1,) + own
        out = pl.pallas_call(
            functools.partial(attn_out_kernel, n, group, hd ** -0.5),
            out_shape=sds((rows, width), BF16),
            in_specs=[HB, VM, VM, VM, VM, VM, VM], out_specs=VM,
            scratch_shapes=[f(own, F32), f(own, F32), f((chunks - 1, n, 2 * per, LANES), F32), pltpu.SMEM((rows,), jnp.int32), DMA,
                            f(pair, F32), f(mls, F32), f(pair, F32), f(mls, F32), f(pair, F32), f(mls, F32),
                            f(sums, F32), f(sums, F32), f(sums, F32), f(sums, F32),
                            ] + [DMA((chunks, nx))] * 16,
            cost_estimate=pl.CostEstimate(flops=30 * 10 ** 9, bytes_accessed=60 * 10 ** 6, transcendentals=0),
            compiler_params=pltpu.CompilerParams(collective_id=1, has_side_effects=True,
                                                 vmem_limit_bytes=20 * 2 ** 20),
            name='attn_out',
        )(hbm[-1], q, k_new, v_new, acc0, ml0, w_out)
        return out, k_new.reshape(k_cache.shape), v_new.reshape(v_cache.shape)

    return jax.shard_map(local_step, mesh=mesh,
                         in_specs=(row_spec, P(), P(), P(), P('sp', None), cache_spec, cache_spec, len_spec, len_spec),
                         out_specs=(row_spec, cache_spec, cache_spec), check_vma=False)
```

```python
import functools

import jax
import jax.numpy as jnp
from jax import lax
from jax.experimental import pallas as pl
from jax.experimental.pallas import tpu as pltpu
from jax.sharding import PartitionSpec as P

MESH = pl.DeviceIdType.MESH
NEG = -3.4e38
LANES = 128
F32 = jnp.float32
BF16 = jnp.bfloat16


def sp_dev(i):
    return {'sp': i}


def rcopy(src, dst, ss, rs, dev):
    return pltpu.make_async_remote_copy(src_ref=src, dst_ref=dst, send_sem=ss, recv_sem=rs,
                                        device_id=sp_dev(dev), device_id_type=MESH)


def qkv_kernel(n, group, chunk, scale, hid_hbm, wq_hbm, wk_hbm, wv_hbm, k_hbm, v_hbm, wp_hbm, vl_hbm,
               q_ref, kv_ref, kb, vb, acc, ml, ra, rml, hid, wq, wkv, qs, kvs, wp, vl, hsem, wsem, csem, isem, ssem, rsem, psend,
               precv, asend, arecv, msend, mrecv):
    nx = n // 2
    me = lax.axis_index('sp')
    x, c = me // 2, lax.rem(me, 2)
    cols = wq.shape[2]
    own = me
    opp = 2 * lax.rem(x + nx // 2, nx) + c
    partner = 2 * x + 1 - c
    ch = pltpu.make_async_copy(hid_hbm, hid, hsem)
    ch.start()
    loads = []
    half = cols // 2
    for i, (blk, lo, size) in enumerate(((own, 0, half), (own, half, half), (opp, 0, cols))):
        cp = pltpu.make_async_copy(wq_hbm.at[:, pl.ds(pl.multiple_of(blk * cols + lo, half), size)],
                                   wq.at[i // 2, :, lo:lo + size], wsem.at[i])
        cp.start()
        loads.append(cp)
    ints = [pltpu.make_async_copy(src, dst, isem.at[i]) for i, (src, dst) in enumerate(((wp_hbm, wp), (vl_hbm, vl)))]
    for cp in ints:
        cp.start()
    near = [lax.rem(x + d, nx) for d in (1, nx - 1)]
    bar = pltpu.get_barrier_semaphore()
    peers = [2 * t + u for t in near for u in range(2)] + [partner]
    for peer in peers:
        pl.semaphore_signal(bar, inc=1, device_id=sp_dev(peer), device_id_type=MESH)
    pick = [pltpu.make_async_copy(w, wkv, wsem.at[3]) for w in (wk_hbm, wv_hbm)]
    for i in range(2):
        @pl.when(c == i)
        def _():
            pick[i].start()

    def project(w):
        return jnp.dot(hid[...], w, preferred_element_type=F32).astype(BF16)

    def part(blk, h):
        return q_ref.at[blk, :, h * half:(h + 1) * half]

    sends = []

    def go(*args):
        sends.append(rcopy(*args))
        sends[-1].start()

    ch.wait()
    loads[0].wait()
    q_ref[own, :, 0:half] = project(wq[0, :, 0:half])
    pl.semaphore_wait(bar, len(peers))
    for d in range(2):
        go(part(own, 0), part(own, 0), ssem.at[d, 0], rsem.at[d, 0], 2 * near[d] + c)
    go(part(own, 0), part(own, 0), psend.at[0], precv.at[0], partner)
    loads[1].wait()
    parts = csem.shape[1]
    step = kb.shape[0] // parts
    caches = []
    for g in range(parts):
        for i, (src, dst) in enumerate(((k_hbm, kb), (v_hbm, vb))):
            cp = pltpu.make_async_copy(src.at[pl.ds(g * step, step)], dst.at[pl.ds(g * step, step)], csem.at[i, g])
            cp.start()
            caches.append(cp)
    q_ref[own, :, half:cols] = project(wq[0, :, half:cols])
    for d in range(2):
        for t in range(2):
            go(part(own, 1), part(own, 1), ssem.at[d, 1 + t], rsem.at[d, 1 + c], 2 * near[d] + t)
    go(part(own, 1), part(own, 1), psend.at[1], precv.at[1], partner)
    loads[2].wait()
    q_ref[opp] = project(wq[1])
    go(q_ref.at[opp], q_ref.at[opp], psend.at[2], precv.at[2], partner)
    pick[0].wait()
    kv_ref[c] = project(wkv[...])
    go(kv_ref.at[c], kv_ref.at[c], psend.at[3], precv.at[3], partner)
    for d in range(2):
        blk = 2 * near[1 - d] + c
        rcopy(part(own, 0), part(blk, 0), ssem.at[d, 0], rsem.at[d, 0], partner).wait_recv()
        go(part(blk, 0), part(blk, 0), psend.at[4 + d], precv.at[4 + d], partner)
    popp = 2 * lax.rem(x + nx // 2, nx) + 1 - c
    for h in range(2):
        rcopy(part(own, h), part(partner, h), psend.at[h], precv.at[h], partner).wait_recv()
    rcopy(q_ref.at[own], q_ref.at[popp], psend.at[2], precv.at[2], partner).wait_recv()
    rcopy(kv_ref.at[c], kv_ref.at[1 - c], psend.at[3], precv.at[3], partner).wait_recv()
    for d in range(2):
        for t in range(2):
            rcopy(part(own, 1), part(2 * near[1 - d] + t, 1), ssem.at[d, 1 + t], rsem.at[d, 1 + t],
                  partner).wait_recv()
        rcopy(part(own, 0), part(2 * near[1 - d] + 1 - c, 0), psend.at[4 + d], precv.at[4 + d], partner).wait_recv()
    for cp in ints + caches[:2]:
        cp.wait()
    kvs[...] = kv_ref[:, 0:chunk, :].astype(F32)
    attend_chunk(qs, q_ref, kb, vb, vl, acc, ml, 0, group, chunk, me * kb.shape[1], scale, (wp, kvs))
    blk = ra.shape[2]
    handed = []
    for d in range(nx):
        j = 2 * lax.rem(x + d, nx) + 1 - c
        handed.append(rcopy(ml.at[j], rml.at[d], msend.at[d], mrecv.at[d], partner))
        handed.append(rcopy(acc.at[:, pl.ds(pl.multiple_of(j * blk, blk), blk)], ra.at[d], asend.at[d], arecv.at[d],
                            partner))
    for cp in handed:
        cp.start()
    for cp in caches[2:]:
        cp.wait()
    for cp in handed:
        cp.wait()
    for cp in sends:
        cp.wait_send()


def stage_q(qs, q_ref, t, chunk, hd):
    per = q_ref.shape[2] // hd
    for h in range(q_ref.shape[0] * per):
        for z in range(hd // LANES):
            lo = (h % per) * hd + z * LANES
            qs[z, h * chunk:(h + 1) * chunk, :] = q_ref[h // per, t * chunk:(t + 1) * chunk, lo:lo + LANES].astype(F32)


def attend(qs, kb, vb, vl, acc, b0, at0, group, chunk, heads, base, scale, m_all, l_all, fresh=None):
    seq, hd = kb.shape[1:]
    halves = hd // LANES
    pos_iota = lax.broadcasted_iota(jnp.int32, (heads, seq), 1)
    lane_iota = lax.broadcasted_iota(jnp.int32, (heads, LANES), 1)
    scores = []
    for r in range(group):
        qb = jnp.concatenate([qs[z, pl.ds(at0 + r, heads, stride=chunk), :] for z in range(halves)], axis=1)
        scores.append(lax.dot_general(qb.astype(BF16), kb[b0 + at0 + r], (((1,), (1,)), ((), ())),
                                      preferred_element_type=F32))
    probs, extra = [], []
    for r in range(group):
        valid = pos_iota < vl[b0 + at0 + r] - base
        s = scores[r]
        if fresh is not None:
            wp, kvs = fresh
            newest = pos_iota == wp[b0 + at0 + r] - base
            qb = jnp.concatenate([qs[z, pl.ds(at0 + r, heads, stride=chunk), :] for z in range(halves)], axis=1)
            s = jnp.where(newest, jnp.sum(qb * kvs[0, pl.ds(at0 + r, 1), :], axis=1, keepdims=True), s)
        s = jnp.where(valid, s * scale, NEG)
        m = jnp.max(s, axis=1, keepdims=True)
        p = jnp.where(valid, jnp.exp(s - m), 0.0)
        l = jnp.sum(p, axis=1, keepdims=True)
        here = lane_iota == at0 + r
        m_all = jnp.where(here, m, m_all)
        l_all = jnp.where(here, l, l_all)
        p = p.astype(BF16)
        if fresh is not None:
            p = p.astype(F32)
            extra.append(jnp.sum(jnp.where(newest, p, 0.0), axis=1, keepdims=True) * kvs[1, pl.ds(at0 + r, 1), :])
            p = jnp.where(newest, 0.0, p).astype(BF16)
        probs.append(p)
    for r in range(group):
        o = jnp.dot(probs[r], vb[b0 + at0 + r], preferred_element_type=F32)
        if fresh is not None:
            o = o + extra[r]
        for z in range(halves):
            acc[z, pl.ds(at0 + r, heads, stride=chunk), :] = o[:, z * LANES:(z + 1) * LANES]
    return m_all, l_all


def attend_chunk(qs, q_ref, kb, vb, vl, acc, ml, t, group, chunk, base, scale, fresh=None):
    n, hd = q_ref.shape[0], kb.shape[2]
    per = q_ref.shape[2] // hd
    heads = n * per
    stage_q(qs, q_ref, t, chunk, hd)

    def step(g, carry):
        return attend(qs, kb, vb, vl, acc, t * chunk, g * group, group, chunk, heads, base, scale, *carry, fresh)

    init = (jnp.full((heads, LANES), NEG, F32), jnp.zeros((heads, LANES), F32))
    m_all, l_all = lax.fori_loop(0, chunk // group, step, init)
    for i in range(n):
        ml[i, 0:per, :] = m_all[i * per:(i + 1) * per]
        ml[i, per:2 * per, :] = l_all[i * per:(i + 1) * per]


def attn_out_kernel(n, group, scale, vl_hbm, q_ref, kb, vb, acc0, ml0, ra0, rml0, w_ref, out_ref, qs, acc, ml, vl, vsem,
                    ra, rml, sb, sml, rb, rbml, sd, rd, se, re,
                    amsend, amrecv, bmsend, bmrecv, asend, arecv, bsend, brecv, dsend, drecv, esend, erecv,
                    fsend, frecv, gsend, grecv):
    nx = n // 2
    me = lax.axis_index('sp')
    x, c = me // 2, lax.rem(me, 2)
    partner = 2 * x + 1 - c
    wide = out_ref.shape[1] // n
    chunks, halves = acc.shape[0] + 1, acc.shape[1]
    blk = acc.shape[2] // n
    chunk = out_ref.shape[0] // chunks
    per = blk // chunk
    heads = per * n
    hd = kb.shape[2]
    far = [2, 1, 3] if nx == 4 else list(range(1, nx))
    near = [1, 3, 2] if nx == 4 else list(range(1, nx))
    order = far + [0]

    def chip(d):
        return lax.rem(x + d, nx)

    bar = pltpu.get_barrier_semaphore()
    peers = [2 * chip(d) + u for d in range(1, nx) for u in range(2)] + [partner]
    for peer in peers:
        pl.semaphore_signal(bar, inc=1, device_id=sp_dev(peer), device_id_type=MESH)
    lens = pltpu.make_async_copy(vl_hbm, vl, vsem)
    lens.start()

    def w_at(j):
        return w_ref[:, pl.ds(pl.multiple_of(j * wide, wide), wide)]

    pending = []

    def go(*args):
        cp = rcopy(*args)
        cp.start()
        pending.append(cp)

    def landed(*args):
        rcopy(*args, partner).wait_recv()

    def acc_at(j):
        return pl.multiple_of(j * blk, blk)

    def local(t):
        attend_chunk(qs.at[t - 1], q_ref, kb, vb, vl, acc.at[t - 1], ml.at[t - 1], t, group, chunk, me * kb.shape[1], scale)

    def acc_of(t):
        return acc.at[t - 1] if t else acc0

    def ml_of(t):
        return ml.at[t - 1] if t else ml0

    def share(t):
        for d in order:
            j = 2 * chip(d) + 1 - c
            go(ml_of(t).at[j], rml.at[t, d], amsend.at[t, d], amrecv.at[t, d], partner)
            go(acc_of(t).at[:, pl.ds(acc_at(j), blk)], ra.at[t, d], asend.at[t, d], arecv.at[t, d], partner)

    def merge(t):
        got, got_ml = (ra.at[t], rml.at[t]) if t else (ra0, rml0)
        for d in order if t else ():
            landed(ml_of(t).at[0], rml.at[t, d], amsend.at[t, d], amrecv.at[t, d])
            landed(ra.at[t, d], ra.at[t, d], asend.at[t, d], arecv.at[t, d])
        for d in order:
            j = 2 * chip(d) + c
            mine, theirs = ml_of(t)[j], got_ml[d]
            m = jnp.maximum(mine[0:per], theirs[0:per])
            fa, fb = jnp.exp(mine[0:per] - m), jnp.exp(theirs[0:per] - m)
            l = fa * mine[per:2 * per] + fb * theirs[per:2 * per]
            f = jnp.transpose(jnp.concatenate([fa, fb, m, l], axis=0))[0:chunk]
            sml[t, d, 0:per, :] = m
            sml[t, d, per:2 * per, :] = l
            for h in range(per):
                r = slice(h * chunk, (h + 1) * chunk)
                for z in range(halves):
                    own = acc_of(t)[z, pl.ds(acc_at(j) + h * chunk, chunk), :]
                    sb[t, d, z, r, :] = own * f[:, h:h + 1] + got[d, z, r, :] * f[:, per + h:per + h + 1]

    def spread(t):
        for d in far:
            j = 2 * chip(d) + c
            go(sml.at[t, d], rbml.at[t, d], bmsend.at[t, d], bmrecv.at[t, d], j)
            go(sb.at[t, d], rb.at[t, d], bsend.at[t, d], brecv.at[t, d], j)

    def pair(t):
        merge(t)
        spread(t)

    def out_at(t, j):
        return out_ref.at[pl.ds(t * chunk, chunk), pl.ds(pl.multiple_of(j * wide, wide), wide)]

    def project(t):
        for d in range(1, nx):
            landed(sml.at[t, d], rbml.at[t, d], bmsend.at[t, d], bmrecv.at[t, d])
            landed(sb.at[t, d], rb.at[t, d], bsend.at[t, d], brecv.at[t, d])
        mls = [sml[t, 0]] + [rbml[t, d] for d in range(1, nx)]
        m = functools.reduce(jnp.maximum, [u[0:per] for u in mls])
        fs = [jnp.exp(u[0:per] - m) for u in mls]
        l = sum(f * u[per:2 * per] for f, u in zip(fs, mls))
        f = jnp.transpose(jnp.concatenate([f / l for f in fs], axis=0))[0:chunk]
        parts = []
        for h in range(per):
            r = slice(h * chunk, (h + 1) * chunk)
            for z in range(halves):
                terms = [sb[t, 0, z, r, :]] + [rb[t, d, z, r, :] for d in range(1, nx)]
                parts.append(sum(u * f[:, d * per + h:d * per + h + 1] for d, u in enumerate(terms)))
        attn = jnp.concatenate(parts, axis=1).astype(BF16)
        for d in order:
            sd[t, d] = jnp.dot(attn, w_at(2 * chip(d) + 1 - c), preferred_element_type=F32)
        for d in order:
            go(sd.at[t, d], rd.at[t, d], dsend.at[t, d], drecv.at[t, d], partner)
        for d in order:
            se[t, d] = jnp.dot(attn, w_at(2 * chip(d) + c), preferred_element_type=F32)

    def reduce(t):
        for d in order:
            landed(sd.at[t, d], rd.at[t, d], dsend.at[t, d], drecv.at[t, d])
        for d in order:
            se[t, d] = se[t, d] + rd[t, d]
        for d in far:
            go(se.at[t, d], re.at[t, d], esend.at[t, d], erecv.at[t, d], 2 * chip(d) + c)

    def finish(t):
        for d in range(1, nx):
            landed(se.at[t, d], re.at[t, d], esend.at[t, d], erecv.at[t, d])
        out_ref[t * chunk:(t + 1) * chunk, pl.ds(pl.multiple_of(me * wide, wide), wide)] = (
            se[t, 0] + sum(re[t, d] for d in range(1, nx))).astype(BF16)
        last = t == chunks - 1
        for d in far:
            go(out_at(t, me), out_at(t, me), fsend.at[t, d], frecv.at[t, d], 2 * chip(d) + c)
            if last:
                go(out_at(t, me), out_at(t, me), gsend.at[t, d], grecv.at[t, d], 2 * chip(d) + 1 - c)
        go(out_at(t, me), out_at(t, me), gsend.at[t, 0], grecv.at[t, 0], partner)

    def forward(t):
        for d in near:
            src = 2 * chip(nx - d) + c
            landed(out_at(t, me), out_at(t, src), fsend.at[t, d], frecv.at[t, d])
            if t < chunks - 1:
                go(out_at(t, src), out_at(t, src), gsend.at[t, d], grecv.at[t, d], partner)

    merge(0)
    lens.wait()
    local(1)
    pl.semaphore_wait(bar, len(peers))
    spread(0)
    share(1)
    for t in range(2, chunks):
        local(t)
        share(t)
        pair(t - 1)
    project(0)
    pair(chunks - 1)
    reduce(0)
    for t in range(1, chunks):
        project(t)
        reduce(t)
    for t in range(chunks):
        finish(t)
    for t in range(chunks):
        forward(t)
    for t in range(chunks):
        for d in [0] + near:
            src = 2 * chip(nx - d if d else 0) + 1 - c
            landed(out_at(t, me), out_at(t, src), gsend.at[t, d], grecv.at[t, d])
    for cp in pending:
        cp.wait_send()


def solution(mesh):
    n = mesh.shape['sp']
    nx = n // 2
    row_spec = P(('rep', 'dp'), None)
    cache_spec = P(('rep', 'dp'), 'sp', None, None)
    len_spec = P(('rep', 'dp'))
    VM = pl.BlockSpec(memory_space=pltpu.VMEM)
    HB = pl.BlockSpec(memory_space=pltpu.HBM)
    SM = pl.BlockSpec(memory_space=pltpu.SMEM)
    DMA = pltpu.SemaphoreType.DMA

    def local_step(hidden, w_query, w_key, w_value, w_out, k_cache, v_cache, write_pos, valid_len):
        rows, seq, kv_heads, hd = k_cache.shape
        width = hidden.shape[1]
        proj = w_query.shape[1]
        heads = proj // hd
        cols = proj // n
        per = heads // n
        k3, v3 = k_cache.reshape(rows, seq, hd), v_cache.reshape(rows, seq, hd)
        sds = jax.ShapeDtypeStruct

        group, chunk = 8, rows // 4
        chunks = rows // chunk
        f = pltpu.VMEM
        halves = hd // LANES
        own = (halves, heads * chunk, LANES)
        hbm = [pltpu.with_memory_space_constraint(u, pltpu.HBM)
               for u in (hidden, w_query, w_key, w_value, k3, v3, write_pos, valid_len)]
        q, kv, kb, vb, acc0, ml0, ra0, rml0 = pl.pallas_call(
            functools.partial(qkv_kernel, n, group, chunk, hd ** -0.5),
            out_shape=(f((n, rows, cols), BF16), f((2, rows, hd), BF16),
                       f((rows, seq, hd), BF16), f((rows, seq, hd), BF16), f(own, F32), f((n, 2 * per, LANES), F32),
                       f((nx, halves, per * chunk, LANES), F32), f((nx, 2 * per, LANES), F32)),
            in_specs=[HB] * 8, out_specs=(VM,) * 8,
            scratch_shapes=[f((rows, width), BF16), f((2, width, cols), BF16), f((width, hd), BF16),
                            f(own, F32), f((2, chunk, hd), F32), pltpu.SMEM((rows,), jnp.int32),
                            pltpu.SMEM((rows,), jnp.int32),
                            DMA, DMA((4,)), DMA((2, chunks)), DMA((2,)), DMA((2, 3)), DMA((2, 3)), DMA((6,)), DMA((6,))] + [DMA((nx,))] * 4,
            compiler_params=pltpu.CompilerParams(collective_id=0, has_side_effects=True,
                                                 vmem_limit_bytes=24 * 2 ** 20),
            name='qkv',
        )(*hbm)

        kv, when = lax.optimization_barrier((kv, write_pos))
        place = lax.axis_index('sp') * seq + jnp.arange(seq, dtype=jnp.int32)
        at_pos = (place[None, :] == when[:, None])[:, :, None]
        k_new = jnp.where(at_pos, kv[0][:, None, :], kb)
        v_new = jnp.where(at_pos, kv[1][:, None, :], vb)

        wide = width // n
        pair = (chunks, nx, halves, per * chunk, LANES)
        sums = (chunks, nx, chunk, wide)
        mls = (chunks, nx, 2 * per, LANES)
        own = (chunks - 1,) + own
        out = pl.pallas_call(
            functools.partial(attn_out_kernel, n, group, hd ** -0.5),
            out_shape=sds((rows, width), BF16),
            in_specs=[HB, VM, VM, VM, VM, VM, VM, VM, VM], out_specs=VM,
            scratch_shapes=[f(own, F32), f(own, F32), f((chunks - 1, n, 2 * per, LANES), F32), pltpu.SMEM((rows,), jnp.int32), DMA,
                            f(pair, F32), f(mls, F32), f(pair, F32), f(mls, F32), f(pair, F32), f(mls, F32),
                            f(sums, F32), f(sums, F32), f(sums, F32), f(sums, F32),
                            ] + [DMA((chunks, nx))] * 16,
            cost_estimate=pl.CostEstimate(flops=30 * 10 ** 9, bytes_accessed=60 * 10 ** 6, transcendentals=0),
            compiler_params=pltpu.CompilerParams(collective_id=1, has_side_effects=True,
                                                 vmem_limit_bytes=20 * 2 ** 20),
            name='attn_out',
        )(hbm[-1], q, k_new, v_new, acc0, ml0, ra0, rml0, w_out)
        return out, k_new.reshape(k_cache.shape), v_new.reshape(v_cache.shape)

    return jax.shard_map(local_step, mesh=mesh,
                         in_specs=(row_spec, P(), P(), P(), P('sp', None), cache_spec, cache_spec, len_spec, len_spec),
                         out_specs=(row_spec, cache_spec, cache_spec), check_vma=False)
```

```python
import functools

import jax
import jax.numpy as jnp
from jax import lax
from jax.experimental import pallas as pl
from jax.experimental.pallas import tpu as pltpu
from jax.sharding import PartitionSpec as P

MESH = pl.DeviceIdType.MESH
NEG = -3.4e38
LANES = 128
F32 = jnp.float32
BF16 = jnp.bfloat16


def sp_dev(i):
    return {'sp': i}


def rcopy(src, dst, ss, rs, dev):
    return pltpu.make_async_remote_copy(src_ref=src, dst_ref=dst, send_sem=ss, recv_sem=rs,
                                        device_id=sp_dev(dev), device_id_type=MESH)


def qkv_kernel(n, group, chunk, scale, hid_hbm, wq_hbm, wk_hbm, wv_hbm, k_hbm, v_hbm, wp_hbm, vl_hbm,
               q_ref, kv_ref, kb, vb, acc, ml, ra, rml, hid, wq, wkv, qs, kvs, wp, vl, hsem, wsem, csem, isem, ssem, rsem, psend,
               precv, asend, arecv, msend, mrecv):
    nx = n // 2
    me = lax.axis_index('sp')
    x, c = me // 2, lax.rem(me, 2)
    cols = wq.shape[2]
    own = me
    opp = 2 * lax.rem(x + nx // 2, nx) + c
    partner = 2 * x + 1 - c
    ch = pltpu.make_async_copy(hid_hbm, hid, hsem)
    ch.start()
    loads = []
    half = cols // 2
    for i, (blk, lo, size) in enumerate(((own, 0, half), (own, half, half), (opp, 0, cols))):
        cp = pltpu.make_async_copy(wq_hbm.at[:, pl.ds(pl.multiple_of(blk * cols + lo, half), size)],
                                   wq.at[i // 2, :, lo:lo + size], wsem.at[i])
        cp.start()
        loads.append(cp)
    ints = [pltpu.make_async_copy(src, dst, isem.at[i]) for i, (src, dst) in enumerate(((wp_hbm, wp), (vl_hbm, vl)))]
    for cp in ints:
        cp.start()
    near = [lax.rem(x + d, nx) for d in (1, nx - 1)]
    bar = pltpu.get_barrier_semaphore()
    peers = [2 * t + u for t in near for u in range(2)] + [partner]
    for peer in peers:
        pl.semaphore_signal(bar, inc=1, device_id=sp_dev(peer), device_id_type=MESH)
    pick = [pltpu.make_async_copy(w, wkv, wsem.at[3]) for w in (wk_hbm, wv_hbm)]
    for i in range(2):
        @pl.when(c == i)
        def _():
            pick[i].start()

    def project(w):
        return jnp.dot(hid[...], w, preferred_element_type=F32).astype(BF16)

    def part(blk, h):
        return q_ref.at[blk, :, h * half:(h + 1) * half]

    sends = []

    def go(*args):
        sends.append(rcopy(*args))
        sends[-1].start()

    ch.wait()
    loads[0].wait()
    q_ref[own, :, 0:half] = project(wq[0, :, 0:half])
    pl.semaphore_wait(bar, len(peers))
    for d in range(2):
        go(part(own, 0), part(own, 0), ssem.at[d, 0], rsem.at[d, 0], 2 * near[d] + c)
    go(part(own, 0), part(own, 0), psend.at[0], precv.at[0], partner)
    loads[1].wait()
    parts = csem.shape[1]
    step = kb.shape[0] // parts
    caches = []
    for g in range(parts):
        for i, (src, dst) in enumerate(((k_hbm, kb), (v_hbm, vb))):
            cp = pltpu.make_async_copy(src.at[pl.ds(g * step, step)], dst.at[pl.ds(g * step, step)], csem.at[i, g])
            cp.start()
            caches.append(cp)
    q_ref[own, :, half:cols] = project(wq[0, :, half:cols])
    for d in range(2):
        for t in range(2):
            go(part(own, 1), part(own, 1), ssem.at[d, 1 + t], rsem.at[d, 1 + c], 2 * near[d] + t)
    go(part(own, 1), part(own, 1), psend.at[1], precv.at[1], partner)
    loads[2].wait()
    q_ref[opp] = project(wq[1])
    go(q_ref.at[opp], q_ref.at[opp], psend.at[2], precv.at[2], partner)
    pick[0].wait()
    kv_ref[c] = project(wkv[...])
    go(kv_ref.at[c], kv_ref.at[c], psend.at[3], precv.at[3], partner)
    for d in range(2):
        blk = 2 * near[1 - d] + c
        rcopy(part(own, 0), part(blk, 0), ssem.at[d, 0], rsem.at[d, 0], partner).wait_recv()
        go(part(blk, 0), part(blk, 0), psend.at[4 + d], precv.at[4 + d], partner)
    popp = 2 * lax.rem(x + nx // 2, nx) + 1 - c
    for h in range(2):
        rcopy(part(own, h), part(partner, h), psend.at[h], precv.at[h], partner).wait_recv()
    rcopy(q_ref.at[own], q_ref.at[popp], psend.at[2], precv.at[2], partner).wait_recv()
    rcopy(kv_ref.at[c], kv_ref.at[1 - c], psend.at[3], precv.at[3], partner).wait_recv()
    for d in range(2):
        for t in range(2):
            rcopy(part(own, 1), part(2 * near[1 - d] + t, 1), ssem.at[d, 1 + t], rsem.at[d, 1 + t],
                  partner).wait_recv()
        rcopy(part(own, 0), part(2 * near[1 - d] + 1 - c, 0), psend.at[4 + d], precv.at[4 + d], partner).wait_recv()
    for cp in ints + caches[:2]:
        cp.wait()
    kvs[...] = kv_ref[:, 0:chunk, :].astype(F32)
    attend_chunk(qs, q_ref, kb, vb, vl, acc, ml, 0, group, chunk, me * kb.shape[1], scale, (wp, kvs))
    blk = ra.shape[2]
    handed = []
    for d in range(nx):
        j = 2 * lax.rem(x + d, nx) + 1 - c
        handed.append(rcopy(ml.at[j], rml.at[d], msend.at[d], mrecv.at[d], partner))
        handed.append(rcopy(acc.at[:, pl.ds(pl.multiple_of(j * blk, blk), blk)], ra.at[d], asend.at[d], arecv.at[d],
                            partner))
    for cp in handed:
        cp.start()
    for cp in caches[2:]:
        cp.wait()
    for cp in handed:
        cp.wait()
    for cp in sends:
        cp.wait_send()


def stage_q(qs, q_ref, t, chunk, hd):
    per = q_ref.shape[2] // hd
    for h in range(q_ref.shape[0] * per):
        for z in range(hd // LANES):
            lo = (h % per) * hd + z * LANES
            qs[z, h * chunk:(h + 1) * chunk, :] = q_ref[h // per, t * chunk:(t + 1) * chunk, lo:lo + LANES].astype(F32)


def attend(qs, kb, vb, vl, acc, b0, at0, group, chunk, heads, base, scale, m_all, l_all, fresh=None):
    seq, hd = kb.shape[1:]
    halves = hd // LANES
    pos_iota = lax.broadcasted_iota(jnp.int32, (heads, seq), 1)
    lane_iota = lax.broadcasted_iota(jnp.int32, (heads, LANES), 1)
    scores = []
    for r in range(group):
        qb = jnp.concatenate([qs[z, pl.ds(at0 + r, heads, stride=chunk), :] for z in range(halves)], axis=1)
        scores.append(lax.dot_general(qb.astype(BF16), kb[b0 + at0 + r], (((1,), (1,)), ((), ())),
                                      preferred_element_type=F32))
    probs, extra = [], []
    for r in range(group):
        valid = pos_iota < vl[b0 + at0 + r] - base
        s = scores[r]
        if fresh is not None:
            wp, kvs = fresh
            newest = pos_iota == wp[b0 + at0 + r] - base
            qb = jnp.concatenate([qs[z, pl.ds(at0 + r, heads, stride=chunk), :] for z in range(halves)], axis=1)
            s = jnp.where(newest, jnp.sum(qb * kvs[0, pl.ds(at0 + r, 1), :], axis=1, keepdims=True), s)
        s = jnp.where(valid, s * scale, NEG)
        m = jnp.max(s, axis=1, keepdims=True)
        p = jnp.where(valid, jnp.exp(s - m), 0.0)
        l = jnp.sum(p, axis=1, keepdims=True)
        here = lane_iota == at0 + r
        m_all = jnp.where(here, m, m_all)
        l_all = jnp.where(here, l, l_all)
        p = p.astype(BF16)
        if fresh is not None:
            p = p.astype(F32)
            extra.append(jnp.sum(jnp.where(newest, p, 0.0), axis=1, keepdims=True) * kvs[1, pl.ds(at0 + r, 1), :])
            p = jnp.where(newest, 0.0, p).astype(BF16)
        probs.append(p)
    for r in range(group):
        o = jnp.dot(probs[r], vb[b0 + at0 + r], preferred_element_type=F32)
        if fresh is not None:
            o = o + extra[r]
        for z in range(halves):
            acc[z, pl.ds(at0 + r, heads, stride=chunk), :] = o[:, z * LANES:(z + 1) * LANES]
    return m_all, l_all


def attend_chunk(qs, q_ref, kb, vb, vl, acc, ml, t, group, chunk, base, scale, fresh=None):
    n, hd = q_ref.shape[0], kb.shape[2]
    per = q_ref.shape[2] // hd
    heads = n * per
    stage_q(qs, q_ref, t, chunk, hd)

    def step(g, carry):
        return attend(qs, kb, vb, vl, acc, t * chunk, g * group, group, chunk, heads, base, scale, *carry, fresh)

    init = (jnp.full((heads, LANES), NEG, F32), jnp.zeros((heads, LANES), F32))
    m_all, l_all = lax.fori_loop(0, chunk // group, step, init)
    for i in range(n):
        ml[i, 0:per, :] = m_all[i * per:(i + 1) * per]
        ml[i, per:2 * per, :] = l_all[i * per:(i + 1) * per]


def attn_out_kernel(n, group, scale, vl_hbm, q_ref, kb, vb, acc0, ml0, ra0, rml0, w_ref, out_ref, qs, acc, ml, vl, vsem,
                    ra, rml, sb, sml, rb, rbml, sd, rd, se, re,
                    amsend, amrecv, bmsend, bmrecv, asend, arecv, bsend, brecv, dsend, drecv, esend, erecv,
                    fsend, frecv, gsend, grecv):
    nx = n // 2
    me = lax.axis_index('sp')
    x, c = me // 2, lax.rem(me, 2)
    partner = 2 * x + 1 - c
    wide = out_ref.shape[1] // n
    chunks, halves = acc.shape[0] + 1, acc.shape[1]
    blk = acc.shape[2] // n
    chunk = out_ref.shape[0] // chunks
    per = blk // chunk
    heads = per * n
    hd = kb.shape[2]
    far = [2, 1, 3] if nx == 4 else list(range(1, nx))
    near = [1, 3, 2] if nx == 4 else list(range(1, nx))
    order = far + [0]

    def chip(d):
        return lax.rem(x + d, nx)

    bar = pltpu.get_barrier_semaphore()
    peers = [2 * chip(d) + u for d in range(1, nx) for u in range(2)] + [partner]
    for peer in peers:
        pl.semaphore_signal(bar, inc=1, device_id=sp_dev(peer), device_id_type=MESH)
    lens = pltpu.make_async_copy(vl_hbm, vl, vsem)
    lens.start()

    def w_at(j):
        return w_ref[:, pl.ds(pl.multiple_of(j * wide, wide), wide)]

    pending = []

    def go(*args):
        cp = rcopy(*args)
        cp.start()
        pending.append(cp)

    def landed(*args):
        rcopy(*args, partner).wait_recv()

    def acc_at(j):
        return pl.multiple_of(j * blk, blk)

    def local(t):
        attend_chunk(qs.at[t - 1], q_ref, kb, vb, vl, acc.at[t - 1], ml.at[t - 1], t, group, chunk, me * kb.shape[1], scale)

    def acc_of(t):
        return acc.at[t - 1] if t else acc0

    def ml_of(t):
        return ml.at[t - 1] if t else ml0

    def share(t):
        for d in order:
            j = 2 * chip(d) + 1 - c
            go(ml_of(t).at[j], rml.at[t, d], amsend.at[t, d], amrecv.at[t, d], partner)
            go(acc_of(t).at[:, pl.ds(acc_at(j), blk)], ra.at[t, d], asend.at[t, d], arecv.at[t, d], partner)

    def merge(t):
        got, got_ml = (ra.at[t], rml.at[t]) if t else (ra0, rml0)
        for d in order if t else ():
            landed(ml_of(t).at[0], rml.at[t, d], amsend.at[t, d], amrecv.at[t, d])
            landed(ra.at[t, d], ra.at[t, d], asend.at[t, d], arecv.at[t, d])
        for d in order:
            j = 2 * chip(d) + c
            mine, theirs = ml_of(t)[j], got_ml[d]
            m = jnp.maximum(mine[0:per], theirs[0:per])
            fa, fb = jnp.exp(mine[0:per] - m), jnp.exp(theirs[0:per] - m)
            l = fa * mine[per:2 * per] + fb * theirs[per:2 * per]
            f = jnp.transpose(jnp.concatenate([fa, fb, m, l], axis=0))[0:chunk]
            sml[t, d, 0:per, :] = m
            sml[t, d, per:2 * per, :] = l
            for h in range(per):
                r = slice(h * chunk, (h + 1) * chunk)
                for z in range(halves):
                    own = acc_of(t)[z, pl.ds(acc_at(j) + h * chunk, chunk), :]
                    sb[t, d, z, r, :] = own * f[:, h:h + 1] + got[d, z, r, :] * f[:, per + h:per + h + 1]

    def spread(t):
        for d in far:
            j = 2 * chip(d) + c
            go(sml.at[t, d], rbml.at[t, d], bmsend.at[t, d], bmrecv.at[t, d], j)
            go(sb.at[t, d], rb.at[t, d], bsend.at[t, d], brecv.at[t, d], j)

    def pair(t):
        merge(t)
        spread(t)

    def out_at(t, j):
        return out_ref.at[pl.ds(t * chunk, chunk), pl.ds(pl.multiple_of(j * wide, wide), wide)]

    def project(t):
        for d in range(1, nx):
            landed(sml.at[t, d], rbml.at[t, d], bmsend.at[t, d], bmrecv.at[t, d])
            landed(sb.at[t, d], rb.at[t, d], bsend.at[t, d], brecv.at[t, d])
        mls = [sml[t, 0]] + [rbml[t, d] for d in range(1, nx)]
        m = functools.reduce(jnp.maximum, [u[0:per] for u in mls])
        fs = [jnp.exp(u[0:per] - m) for u in mls]
        l = sum(f * u[per:2 * per] for f, u in zip(fs, mls))
        f = jnp.transpose(jnp.concatenate([f / l for f in fs], axis=0))[0:chunk]
        parts = []
        for h in range(per):
            r = slice(h * chunk, (h + 1) * chunk)
            for z in range(halves):
                terms = [sb[t, 0, z, r, :]] + [rb[t, d, z, r, :] for d in range(1, nx)]
                parts.append(sum(u * f[:, d * per + h:d * per + h + 1] for d, u in enumerate(terms)))
        attn = jnp.concatenate(parts, axis=1).astype(BF16)
        for d in order:
            sd[t, d] = jnp.dot(attn, w_at(2 * chip(d) + 1 - c), preferred_element_type=F32)
        for d in order:
            go(sd.at[t, d], rd.at[t, d], dsend.at[t, d], drecv.at[t, d], partner)
        for d in order:
            se[t, d] = jnp.dot(attn, w_at(2 * chip(d) + c), preferred_element_type=F32)

    def reduce(t):
        for d in order:
            landed(sd.at[t, d], rd.at[t, d], dsend.at[t, d], drecv.at[t, d])
        for d in order:
            se[t, d] = se[t, d] + rd[t, d]
        for d in far:
            go(se.at[t, d], re.at[t, d], esend.at[t, d], erecv.at[t, d], 2 * chip(d) + c)

    def finish(t):
        for d in range(1, nx):
            landed(se.at[t, d], re.at[t, d], esend.at[t, d], erecv.at[t, d])
        out_ref[t * chunk:(t + 1) * chunk, pl.ds(pl.multiple_of(me * wide, wide), wide)] = (
            se[t, 0] + sum(re[t, d] for d in range(1, nx))).astype(BF16)
        last = t == chunks - 1
        for d in far:
            go(out_at(t, me), out_at(t, me), fsend.at[t, d], frecv.at[t, d], 2 * chip(d) + c)
            if last:
                go(out_at(t, me), out_at(t, me), gsend.at[t, d], grecv.at[t, d], 2 * chip(d) + 1 - c)
        go(out_at(t, me), out_at(t, me), gsend.at[t, 0], grecv.at[t, 0], partner)

    def forward(t):
        for d in near:
            src = 2 * chip(nx - d) + c
            landed(out_at(t, me), out_at(t, src), fsend.at[t, d], frecv.at[t, d])
            if t < chunks - 1:
                go(out_at(t, src), out_at(t, src), gsend.at[t, d], grecv.at[t, d], partner)

    merge(0)
    lens.wait()
    local(1)
    pl.semaphore_wait(bar, len(peers))
    spread(0)
    share(1)
    for t in range(2, chunks):
        local(t)
        share(t)
        pair(t - 1)
    project(0)
    pair(chunks - 1)
    reduce(0)
    for t in range(1, chunks):
        project(t)
        reduce(t)
    sent = len(pending)
    for t in range(chunks):
        if t == chunks - 1:
            for cp in pending[:sent]:
                cp.wait_send()
        finish(t)
    for t in range(chunks):
        forward(t)
    for t in range(chunks):
        for d in [0] + near:
            src = 2 * chip(nx - d if d else 0) + 1 - c
            landed(out_at(t, me), out_at(t, src), gsend.at[t, d], grecv.at[t, d])
    for cp in pending[sent:]:
        cp.wait_send()


def solution(mesh):
    n = mesh.shape['sp']
    nx = n // 2
    row_spec = P(('rep', 'dp'), None)
    cache_spec = P(('rep', 'dp'), 'sp', None, None)
    len_spec = P(('rep', 'dp'))
    VM = pl.BlockSpec(memory_space=pltpu.VMEM)
    HB = pl.BlockSpec(memory_space=pltpu.HBM)
    SM = pl.BlockSpec(memory_space=pltpu.SMEM)
    DMA = pltpu.SemaphoreType.DMA

    def local_step(hidden, w_query, w_key, w_value, w_out, k_cache, v_cache, write_pos, valid_len):
        rows, seq, kv_heads, hd = k_cache.shape
        width = hidden.shape[1]
        proj = w_query.shape[1]
        heads = proj // hd
        cols = proj // n
        per = heads // n
        k3, v3 = k_cache.reshape(rows, seq, hd), v_cache.reshape(rows, seq, hd)
        sds = jax.ShapeDtypeStruct

        group, chunk = 8, rows // 4
        chunks = rows // chunk
        f = pltpu.VMEM
        halves = hd // LANES
        own = (halves, heads * chunk, LANES)
        hbm = [pltpu.with_memory_space_constraint(u, pltpu.HBM)
               for u in (hidden, w_query, w_key, w_value, k3, v3, write_pos, valid_len)]
        q, kv, kb, vb, acc0, ml0, ra0, rml0 = pl.pallas_call(
            functools.partial(qkv_kernel, n, group, chunk, hd ** -0.5),
            out_shape=(f((n, rows, cols), BF16), f((2, rows, hd), BF16),
                       f((rows, seq, hd), BF16), f((rows, seq, hd), BF16), f(own, F32), f((n, 2 * per, LANES), F32),
                       f((nx, halves, per * chunk, LANES), F32), f((nx, 2 * per, LANES), F32)),
            in_specs=[HB] * 8, out_specs=(VM,) * 8,
            scratch_shapes=[f((rows, width), BF16), f((2, width, cols), BF16), f((width, hd), BF16),
                            f(own, F32), f((2, chunk, hd), F32), pltpu.SMEM((rows,), jnp.int32),
                            pltpu.SMEM((rows,), jnp.int32),
                            DMA, DMA((4,)), DMA((2, chunks)), DMA((2,)), DMA((2, 3)), DMA((2, 3)), DMA((6,)), DMA((6,))] + [DMA((nx,))] * 4,
            compiler_params=pltpu.CompilerParams(collective_id=0, has_side_effects=True,
                                                 vmem_limit_bytes=24 * 2 ** 20),
            name='qkv',
        )(*hbm)

        kv, when = lax.optimization_barrier((kv, write_pos))
        place = lax.axis_index('sp') * seq + jnp.arange(seq, dtype=jnp.int32)
        at_pos = (place[None, :] == when[:, None])[:, :, None]
        k_new = jnp.where(at_pos, kv[0][:, None, :], kb)
        v_new = jnp.where(at_pos, kv[1][:, None, :], vb)

        wide = width // n
        pair = (chunks, nx, halves, per * chunk, LANES)
        sums = (chunks, nx, chunk, wide)
        mls = (chunks, nx, 2 * per, LANES)
        own = (chunks - 1,) + own
        out = pl.pallas_call(
            functools.partial(attn_out_kernel, n, group, hd ** -0.5),
            out_shape=sds((rows, width), BF16),
            in_specs=[HB, VM, VM, VM, VM, VM, VM, VM, VM], out_specs=VM,
            scratch_shapes=[f(own, F32), f(own, F32), f((chunks - 1, n, 2 * per, LANES), F32), pltpu.SMEM((rows,), jnp.int32), DMA,
                            f(pair, F32), f(mls, F32), f(pair, F32), f(mls, F32), f(pair, F32), f(mls, F32),
                            f(sums, F32), f(sums, F32), f(sums, F32), f(sums, F32),
                            ] + [DMA((chunks, nx))] * 16,
            cost_estimate=pl.CostEstimate(flops=30 * 10 ** 9, bytes_accessed=60 * 10 ** 6, transcendentals=0),
            compiler_params=pltpu.CompilerParams(collective_id=1, has_side_effects=True,
                                                 vmem_limit_bytes=20 * 2 ** 20),
            name='attn_out',
        )(hbm[-1], q, k_new, v_new, acc0, ml0, ra0, rml0, w_out)
        return out, k_new.reshape(k_cache.shape), v_new.reshape(v_cache.shape)

    return jax.shard_map(local_step, mesh=mesh,
                         in_specs=(row_spec, P(), P(), P(), P('sp', None), cache_spec, cache_spec, len_spec, len_spec),
                         out_specs=(row_spec, cache_spec, cache_spec), check_vma=False)
```
